32 devices in a mesh: dp: 2 (over x), pool: 4 (over z), ep: 4 (over y, core).
Axes of the slice: x: 2, y: 2, z: 4, core: 2. Of those that a mesh axis runs over, the one named last changes fastest.
Arguments:
- hidden: bfloat16 [2048, 1536], P(('dp', 'ep')), parts along dimension 0
- k_cache: bfloat16 [2, 2048, 128, 2, 128], P(None, ('dp', 'ep')), parts along dimension 1
- v_cache: bfloat16 [2, 2048, 128, 2, 128], P(None, ('dp', 'ep')), parts along dimension 1
- lengths: int32 [2048], P(('dp', 'ep')), parts along dimension 0
- expert_ids: int32 [2, 2048, 2], P(None, ('dp', 'ep')), parts along dimension 1
- w_query: bfloat16 [2, 1536, 1536], replicated
- w_key: bfloat16 [2, 1536, 256], replicated
- w_value: bfloat16 [2, 1536, 256], replicated
- w_out: bfloat16 [2, 1536, 1536], replicated
- w_router: float32 [2, 1536, 8], replicated
- w_gate: bfloat16 [2, 8, 1536, 4096], P(None, 'ep')
- w_up: bfloat16 [2, 8, 1536, 4096], P(None, 'ep')
- w_down: bfloat16 [2, 8, 4096, 1536], P(None, 'ep')
Outputs:
- output: bfloat16 [2048, 1536], P(('dp', 'ep')), parts along dimension 0
There are 2 independent parts. The reference program is written for one: setup_inputs(seed, part) draws one part's arguments, and reference() takes and returns one part's arrays. A program takes and returns all parts, laid end to end along the dimension named above; an argument that names none is the same for every part.
All inputs are finite; a program needn't handle non-finite values.
Results may differ from the reference program's by a relative error of at most 0.0190241.
Values are sent between devices in bfloat16 or wider.
A program may use at most 1 GiB of HBM per device.

```python
import math
import jax
import jax.numpy as jnp
from jax import lax

LAYERS = 2
D = 1536
FF = 4096
EXPERTS = 8
TOPK = 2
HEADS = 12
KV_HEADS = 2
HEAD = 128
TOK = 128
SEQ = 128
NATT = 8
CAP = 96

EPSILON = 1e-6
ROPE_BASE = 10000.0


def draw_routing(key):
    total = TOK * TOPK
    layers_ids = []
    for layer in range(LAYERS):
        key_hot, key_dev = jax.random.split(jax.random.fold_in(key, layer))
        order = jax.random.permutation(key_hot, EXPERTS)
        n_hot = layer + 1
        n_cold = EXPERTS - n_hot
        spare = total - n_hot * CAP
        base_count = spare // n_cold
        extra_count = spare % n_cold

        def one_block(block_key):
            key_rank, key_tok = jax.random.split(block_key)
            ranks = jax.random.permutation(key_rank, n_cold)
            cold_counts = base_count + (ranks < extra_count).astype(jnp.int32)
            counts = jnp.zeros((EXPERTS,), jnp.int32).at[order[:n_hot]].set(CAP).at[order[n_hot:]].set(cold_counts)
            bounds = jnp.cumsum(counts)
            flat = jnp.sum((bounds[None, :] <= jnp.arange(total)[:, None]).astype(jnp.int32), axis=1)
            table = flat.reshape(TOPK, TOK).T
            return table[jax.random.permutation(key_tok, TOK)]

        block_ids = jax.vmap(one_block)(jax.random.split(key_dev, NATT))
        layers_ids.append(block_ids.reshape(NATT * TOK, TOPK))
    return jnp.stack(layers_ids)


def draw_lengths(key):
    tok_total = NATT * TOK
    key_exp, key_len, key_full = jax.random.split(key, 3)
    top_exp = int(math.log2(SEQ))
    exponent = jax.random.randint(key_exp, (tok_total,), 0, top_exp + 1)
    span = jnp.left_shift(jnp.ones((tok_total,), jnp.int32), exponent)
    lens = 1 + jax.random.randint(key_len, (tok_total,), 0, span)
    return lens.at[jax.random.randint(key_full, (), 0, tok_total)].set(SEQ)


def setup_inputs(seed: int = 0, part: int = 0) -> dict:
    tok_total = NATT * TOK
    base_key = jax.random.key(seed)
    part_key = jax.random.fold_in(jax.random.key(seed + 1), part)
    key_hid, key_kc, key_vc, key_len, key_ids = jax.random.split(part_key, 5)
    keys_w = jax.random.split(base_key, 8)

    def gauss(key, shape, scale):
        return jax.random.normal(key, shape, jnp.float32) * scale

    return {
        "hidden": gauss(key_hid, (tok_total, D), 1.0).astype(jnp.bfloat16),
        "k_cache": gauss(key_kc, (LAYERS, tok_total, SEQ, KV_HEADS, HEAD), 1.0).astype(jnp.bfloat16),
        "v_cache": gauss(key_vc, (LAYERS, tok_total, SEQ, KV_HEADS, HEAD), 1.0).astype(jnp.bfloat16),
        "lengths": draw_lengths(key_len),
        "expert_ids": draw_routing(key_ids),
        "w_query": gauss(keys_w[0], (LAYERS, D, HEADS * HEAD), 1.5 * D ** -0.5).astype(jnp.bfloat16),
        "w_key": gauss(keys_w[1], (LAYERS, D, KV_HEADS * HEAD), D ** -0.5).astype(jnp.bfloat16),
        "w_value": gauss(keys_w[2], (LAYERS, D, KV_HEADS * HEAD), D ** -0.5).astype(jnp.bfloat16),
        "w_out": gauss(keys_w[3], (LAYERS, HEADS * HEAD, D), 2.0 * (HEADS * HEAD) ** -0.5).astype(jnp.bfloat16),
        "w_router": gauss(keys_w[4], (LAYERS, D, EXPERTS), 1.5 * D ** -0.5),
        "w_gate": gauss(keys_w[5], (LAYERS, EXPERTS, D, FF), D ** -0.5).astype(jnp.bfloat16),
        "w_up": gauss(keys_w[6], (LAYERS, EXPERTS, D, FF), D ** -0.5).astype(jnp.bfloat16),
        "w_down": gauss(keys_w[7], (LAYERS, EXPERTS, FF, D), 2.0 * FF ** -0.5).astype(jnp.bfloat16),
    }


def rms_normed(values):
    return values * lax.rsqrt(jnp.mean(values * values, axis=-1, keepdims=True) + EPSILON)


def rotary(vectors, positions):
    half = vectors.shape[-1] // 2
    freqs = ROPE_BASE ** (-2.0 * jnp.arange(half, dtype=jnp.float32) / vectors.shape[-1])
    angle = positions[:, None, None] * freqs[None, None, :]
    cosine = jnp.cos(angle)
    sine = jnp.sin(angle)
    first = vectors[..., :half]
    second = vectors[..., half:]
    return jnp.concatenate([first * cosine - second * sine, second * cosine + first * sine], axis=-1)


def attend_block(hidden_blk, keys_blk, vals_blk, lens_blk, w_q, w_k, w_v, w_o):
    hidden_f = hidden_blk.astype(jnp.float32)
    normed = rms_normed(hidden_f).astype(jnp.bfloat16)
    positions = lens_blk.astype(jnp.float32)
    query = rotary(jnp.dot(normed, w_q, preferred_element_type=jnp.float32).reshape(TOK, HEADS, HEAD), positions)
    query = query.astype(jnp.bfloat16).reshape(TOK, KV_HEADS, HEADS // KV_HEADS, HEAD).astype(jnp.float32)
    key_new = rotary(jnp.dot(normed, w_k, preferred_element_type=jnp.float32).reshape(TOK, KV_HEADS, HEAD), positions)
    key_new = key_new.astype(jnp.bfloat16).astype(jnp.float32)
    val_new = jnp.dot(normed, w_v, preferred_element_type=jnp.float32).astype(jnp.bfloat16).reshape(TOK, KV_HEADS, HEAD)
    scale = HEAD ** -0.5
    scores = jnp.einsum("tkgd,tskd->tkgs", query, keys_blk.astype(jnp.float32)) * scale
    valid = jnp.arange(SEQ)[None, None, None, :] < lens_blk[:, None, None, None]
    scores = jnp.where(valid, scores, -jnp.inf)
    score_new = jnp.einsum("tkgd,tkd->tkg", query, key_new) * scale
    peak = jnp.maximum(jnp.max(scores, axis=-1), score_new)
    weights = jnp.exp(scores - peak[..., None])
    weight_new = jnp.exp(score_new - peak)
    denominator = jnp.sum(weights, axis=-1) + weight_new
    mixed = jnp.einsum("tkgs,tskd->tkgd", weights.astype(jnp.bfloat16).astype(jnp.float32), vals_blk.astype(jnp.float32))
    mixed = mixed + weight_new.astype(jnp.bfloat16).astype(jnp.float32)[..., None] * val_new.astype(jnp.float32)[:, :, None, :]
    attended = (mixed / denominator[..., None]).astype(jnp.bfloat16).reshape(TOK, HEADS * HEAD)
    return (hidden_f + jnp.dot(attended, w_o, preferred_element_type=jnp.float32)).astype(jnp.bfloat16)


def moe_layer(attn_out, ids_layer, w_r, w_gate, w_up, w_down):
    residual = attn_out.astype(jnp.float32)
    mixed_in = rms_normed(residual).astype(jnp.bfloat16)
    logits = jnp.dot(mixed_in.astype(jnp.float32), w_r)
    gates = jax.nn.softmax(jnp.take_along_axis(logits, ids_layer, axis=1), axis=-1)
    blocks_in = mixed_in.reshape(NATT, TOK, D).astype(jnp.float32)
    id_blocks = ids_layer.reshape(NATT, TOK, TOPK)
    gate_blocks = gates.reshape(NATT, TOK, TOPK)
    slot_ids = jnp.arange(CAP)

    def step(total_acc, layer_pack):
        expert, w_one, w_three, w_two = layer_pack
        hit = id_blocks == expert
        weight = jnp.sum(jnp.where(hit, gate_blocks, 0.0), axis=2)
        chosen = jnp.any(hit, axis=2)
        rank = jnp.cumsum(chosen.astype(jnp.int32), axis=1) - 1
        select = ((rank[:, None, :] == slot_ids[None, :, None]) & chosen[:, None, :]).astype(jnp.float32)
        rows = jnp.einsum("bct,btd->bcd", select, blocks_in).astype(jnp.bfloat16).reshape(NATT * CAP, D)
        inner = jax.nn.silu(jnp.dot(rows, w_one, preferred_element_type=jnp.float32)) * jnp.dot(rows, w_three, preferred_element_type=jnp.float32)
        result = jnp.dot(inner.astype(jnp.bfloat16), w_two, preferred_element_type=jnp.float32).astype(jnp.bfloat16)
        back = jnp.einsum("bct,bcd->btd", select, result.reshape(NATT, CAP, D).astype(jnp.float32))
        return total_acc + weight[:, :, None] * back, None

    total_acc, _ = lax.scan(step, jnp.zeros((NATT, TOK, D), jnp.float32), (jnp.arange(EXPERTS), w_gate, w_up, w_down))
    return (residual + total_acc.reshape(NATT * TOK, D)).astype(jnp.bfloat16)


def reference(hidden, k_cache, v_cache, lengths, expert_ids, w_query, w_key, w_value, w_out, w_router, w_gate, w_up, w_down):
    def layer_step(state, layer_pack):
        cache_k, cache_v, ids_layer, w_q, w_k, w_v, w_o, w_r, w_one, w_three, w_two = layer_pack

        def per_block(block_in):
            return attend_block(block_in[0], block_in[1], block_in[2], block_in[3], w_q, w_k, w_v, w_o)

        attn_out = lax.map(per_block, (state.reshape(NATT, TOK, D), cache_k.reshape(NATT, TOK, SEQ, KV_HEADS, HEAD), cache_v.reshape(NATT, TOK, SEQ, KV_HEADS, HEAD), lengths.reshape(NATT, TOK)))
        return moe_layer(attn_out.reshape(NATT * TOK, D), ids_layer, w_r, w_one, w_three, w_two), None

    final, _ = lax.scan(layer_step, hidden, (k_cache, v_cache, expert_ids, w_query, w_key, w_value, w_out, w_router, w_gate, w_up, w_down))
    return final
```

```python
import functools
import math

import jax
import jax.numpy as jnp
import numpy as np
from jax import lax
from jax.experimental import pallas as pl
from jax.experimental.pallas import tpu as pltpu
from jax.sharding import PartitionSpec as P

EPSILON = 1e-6
ROPE_BASE = 10000.0
MESH = pl.DeviceIdType.MESH
HEAD = 128
KV = 2
LANES = 128
CHUNK = 512
GU_SLOTS = 5
DOWN_SLOTS = 3
KV_BLOCKS = 4
UNROLL = 4


def rotary_tables(size):
    half = HEAD // 2
    freqs = np.float32(ROPE_BASE) ** (np.float32(-2.0) * np.arange(half, dtype=np.float32) / np.float32(HEAD))
    angle = np.arange(size, dtype=np.float32)[:, None] * freqs[None, :].astype(np.float32)
    cosine = np.cos(angle).astype(np.float32)
    sine = np.sin(angle).astype(np.float32)
    return np.concatenate([cosine, cosine], 1), np.concatenate([-sine, sine], 1)


def normed(values):
    return values * lax.rsqrt(jnp.mean(values * values, axis=-1, keepdims=True) + EPSILON)


def kernel(dims, lens, ids, hid, kc, vc, wq, wk, wv, wo, wr, cos_t, sin_t, wg, wu, wd, out,
           wq_b, wkv_b, wo_b, kbuf, vbuf, gu, dbuf, ubuf, inner, stage, part_l, part_m, merged, far, xg, acc_a,
           q2d, k2d, v2d, o2d, att, gbuf, gsel, wr_b, cosb, sinb, cosr, sinr, id_b,
           wsem, kvsem, gusem, dsem, isem, us, ur, gs, gr, ps, pr, ms, mr, fs, fr, zs, zr, osem):
    layers, toks, model, ff, heads, local = dims
    e = lax.axis_index("ep")
    p = lax.axis_index("pool")
    pools = 4
    partner = e + 1 - 2 * (e % 2)
    cross = (e + 2) % 4
    start = p * toks
    ff_chunks = ff // CHUNK
    gu_total = local * ff_chunks
    d_chunks = model // CHUNK
    d_total = d_chunks * local
    rows = 4 * toks
    group = heads // KV
    seq2 = kbuf.shape[1]
    per_block = toks // KV_BLOCKS

    def remote(src, dst, ssem, rsem, axis, index):
        return pltpu.make_async_remote_copy(src_ref=src, dst_ref=dst, send_sem=ssem, recv_sem=rsem,
                                            device_id={axis: index}, device_id_type=MESH)

    def gu_copies(g):
        layer, i, slot = g // gu_total, g % gu_total, g % GU_SLOTS
        expert, c = i // ff_chunks, i % ff_chunks
        cols = pl.ds(pl.multiple_of(c * CHUNK, CHUNK), CHUNK)
        return [pltpu.make_async_copy(w.at[layer, expert, :, cols], gu.at[slot, k], gusem.at[slot, k])
                for k, w in enumerate((wg, wu))]

    def d_copy(d):
        layer, i, slot = d // d_total, d % d_total, d % DOWN_SLOTS
        j, expert = i // local, i % local
        cols = pl.ds(pl.multiple_of(j * CHUNK, CHUNK), CHUNK)
        return pltpu.make_async_copy(wd.at[layer, expert, :, cols], dbuf.at[slot], dsem.at[slot])

    kvw = KV * HEAD

    def weight_copies(layer):
        return [pltpu.make_async_copy(wq.at[layer], wq_b, wsem.at[0]),
                pltpu.make_async_copy(wk.at[layer], wkv_b.at[:, pl.ds(0, kvw)], wsem.at[1]),
                pltpu.make_async_copy(wv.at[layer], wkv_b.at[:, pl.ds(kvw, kvw)], wsem.at[2]),
                pltpu.make_async_copy(wo.at[layer], wo_b, wsem.at[3])]

    def kv_copies(layer, b):
        here = pl.ds(start + b * per_block, per_block)
        there = pl.ds(b * per_block, per_block)
        return [pltpu.make_async_copy(kc.at[layer, here], kbuf.at[there], kvsem.at[b, 0]),
                pltpu.make_async_copy(vc.at[layer, here], vbuf.at[there], kvsem.at[b, 1])]

    def start_attention(layer):
        copies = weight_copies(layer)
        for c in copies[:3]:
            c.start()
        for b in range(KV_BLOCKS):
            for c in kv_copies(layer, b):
                c.start()
        copies[3].start()

    first = [pltpu.make_async_copy(hid.at[pl.ds(start, toks)], acc_a, isem.at[0]),
             pltpu.make_async_copy(wr, wr_b, isem.at[1]),
             pltpu.make_async_copy(cos_t, cosb, isem.at[2]),
             pltpu.make_async_copy(sin_t, sinb, isem.at[3])]
    for c in first:
        c.start()
    start_attention(0)
    for g in range(GU_SLOTS):
        for c in gu_copies(g):
            c.start()
    for d in range(DOWN_SLOTS):
        d_copy(d).start()

    barrier = pltpu.get_barrier_semaphore()
    pl.semaphore_signal(barrier, inc=1, device_id={"ep": partner}, device_id_type=MESH)
    pl.semaphore_signal(barrier, inc=1, device_id={"ep": cross}, device_id_type=MESH)

    @pl.when(p > 0)
    def _():
        pl.semaphore_signal(barrier, inc=1, device_id={"pool": p - 1}, device_id_type=MESH)

    @pl.when(p < pools - 1)
    def _():
        pl.semaphore_signal(barrier, inc=1, device_id={"pool": p + 1}, device_id_type=MESH)

    middle = (p > 0) & (p < pools - 1)

    @pl.when(middle)
    def _():
        pl.semaphore_wait(barrier, 4)

    @pl.when(jnp.logical_not(middle))
    def _():
        pl.semaphore_wait(barrier, 3)

    for c in first:
        c.wait()

    zeros = jnp.zeros(((16 - heads) * toks, HEAD), jnp.float32)
    for ref in (q2d, k2d, v2d):
        ref[pl.ds(heads * toks, (16 - heads) * toks), :] = zeros

    def spread(t, carry):
        where = pl.ds(t, 1)
        n = lens[start + t]
        cosr[where, :] = cosb[pl.ds(n, 1), :]
        sinr[where, :] = sinb[pl.ds(n, 1), :]
        for layer in range(layers):
            for k in range(2):
                id_b[layer, k, where, :] = jnp.full((1, LANES), ids[layer, k, start + t], jnp.int32)
        return carry

    lax.fori_loop(0, toks, spread, 0)

    lane = lax.broadcasted_iota(jnp.int32, (16, seq2), 1)
    head_kv = jnp.where(lax.broadcasted_iota(jnp.int32, (16, seq2), 0) >= group, 1, 0)
    parity = (lane % KV) == head_kv
    scale = HEAD ** -0.5

    def layer_body(layer, carry):
        hidden = acc_a[...].astype(jnp.float32)
        h = normed(hidden).astype(jnp.bfloat16)
        copies = weight_copies(layer)
        copies[0].wait()
        cosine, sine = cosr[...], sinr[...]

        def rope(v):
            return (v * cosine + pltpu.roll(v, HEAD // 2, 1) * sine).astype(jnp.bfloat16).astype(jnp.float32)

        for n in range(heads * HEAD // CHUNK):
            qn = jnp.dot(h, wq_b[:, n * CHUNK:(n + 1) * CHUNK], preferred_element_type=jnp.float32)
            for k in range(CHUNK // HEAD):
                head = n * (CHUNK // HEAD) + k
                q2d[pl.ds(head * toks, toks), :] = rope(qn[:, k * HEAD:(k + 1) * HEAD])
        copies[1].wait()
        copies[2].wait()
        kv = jnp.dot(h, wkv_b[...], preferred_element_type=jnp.float32)
        for j in range(KV):
            kj = rope(kv[:, j * HEAD:(j + 1) * HEAD])
            vj = kv[:, kvw + j * HEAD:kvw + (j + 1) * HEAD].astype(jnp.bfloat16).astype(jnp.float32)
            for k in range(group):
                at = pl.ds((j * group + k) * toks, toks)
                k2d[at, :] = kj
                v2d[at, :] = vj

        def one_token(t):
            at = pl.ds(t, 16, stride=toks)
            q = q2d[at, :]
            n2 = lens[start + t] * KV
            s = lax.dot_general(q.astype(jnp.bfloat16), kbuf[t], (((1,), (1,)), ((), ())),
                                preferred_element_type=jnp.float32) * scale
            s = jnp.where(parity & (lane < n2), s, -jnp.inf)
            s_new = jnp.sum(q * k2d[at, :], axis=1, keepdims=True) * scale
            peak = jnp.maximum(jnp.max(s, axis=1, keepdims=True), s_new)
            w = jnp.exp(s - peak)
            w_new = jnp.exp(s_new - peak)
            total = jnp.sum(w, axis=1, keepdims=True) + w_new
            o = jnp.dot(w.astype(jnp.bfloat16), vbuf[t], preferred_element_type=jnp.float32)
            o = o + w_new.astype(jnp.bfloat16).astype(jnp.float32) * v2d[at, :]
            o2d[at, :] = o / total

        for b in range(KV_BLOCKS):
            for c in kv_copies(layer, b):
                c.wait()

            def some_tokens(i, carry, b=b):
                for k in range(UNROLL):
                    one_token(b * per_block + i * UNROLL + k)
                return carry

            lax.fori_loop(0, per_block // UNROLL, some_tokens, 0)

        for head in range(heads):
            att[:, head * HEAD:(head + 1) * HEAD] = o2d[pl.ds(head * toks, toks), :].astype(jnp.bfloat16)
        copies[3].wait()
        mean_sq = jnp.zeros((toks, 1), jnp.float32)
        for n in range(model // CHUNK):
            cols = slice(n * CHUNK, (n + 1) * CHUNK)
            a = acc_a[:, cols].astype(jnp.float32) + jnp.dot(att[...], wo_b[:, cols], preferred_element_type=jnp.float32)
            acc_a[:, cols] = a.astype(jnp.bfloat16)

        u = normed(acc_a[...].astype(jnp.float32)).astype(jnp.bfloat16)
        ubuf[layer, pl.ds(0, toks), :] = u

        def block(ref, b):
            return ref.at[layer, pl.ds(b * toks, toks)]

        u_near = remote(block(ubuf, 0), block(ubuf, 1), us.at[0], ur.at[layer, 0], "ep", partner)
        u_far = remote(block(ubuf, 0), block(ubuf, 2), us.at[1], ur.at[layer, 1], "ep", cross)
        u_pass = remote(block(ubuf, 2), block(ubuf, 3), us.at[2], ur.at[layer, 2], "ep", partner)
        g_near = remote(block(gbuf, 0), block(gbuf, 1), gs.at[0], gr.at[layer, 0], "ep", partner)
        g_far = remote(block(gbuf, 0), block(gbuf, 2), gs.at[1], gr.at[layer, 1], "ep", cross)
        g_pass = remote(block(gbuf, 2), block(gbuf, 3), gs.at[2], gr.at[layer, 2], "ep", partner)
        u_far.start()
        u_near.start()

        wl = wr_b[layer]
        hi = wl.astype(jnp.bfloat16).astype(jnp.float32)
        rest = wl - hi
        mid = rest.astype(jnp.bfloat16).astype(jnp.float32)
        low = rest - mid
        wide = jnp.concatenate([hi, mid, low, jnp.zeros((LANES - 3 * wl.shape[0], model), jnp.float32)], axis=0).astype(jnp.bfloat16)
        parts = lax.dot_general(u, wide, (((1,), (1,)), ((), ())), preferred_element_type=jnp.float32)
        logits = parts + pltpu.roll(parts, LANES - 8, 1) + pltpu.roll(parts, LANES - 16, 1)
        expert_lane = lax.broadcasted_iota(jnp.int32, (toks, LANES), 1)
        chosen = (id_b[layer, 0] == expert_lane) | (id_b[layer, 1] == expert_lane)
        logits = jnp.where(chosen, logits, -jnp.inf)
        ew = jnp.exp(logits - jnp.max(logits, axis=1, keepdims=True))
        gbuf[layer, pl.ds(0, toks), :] = ew / jnp.sum(ew, axis=1, keepdims=True)
        g_far.start()
        g_near.start()
        u_far.wait_recv()
        u_pass.start()
        g_far.wait_recv()
        g_pass.start()
        for c in (u_near, u_pass, g_near, g_pass):
            c.wait_recv()

        gates = gbuf[layer]
        row_lane = lax.broadcasted_iota(jnp.int32, (rows, LANES), 1)
        for k in range(local):
            one = jnp.sum(jnp.where(row_lane == e * local + k, gates, 0.0), axis=1, keepdims=True)
            gsel[k] = jnp.broadcast_to(one, (rows, LANES))

        def gu_body(i, carry):
            g = layer * gu_total + i
            slot = g % GU_SLOTS
            for c in gu_copies(g):
                c.wait()
            tokens = ubuf[layer]
            one = jnp.dot(tokens, gu[slot, 0], preferred_element_type=jnp.float32)
            three = jnp.dot(tokens, gu[slot, 1], preferred_element_type=jnp.float32)
            cols = pl.ds(pl.multiple_of((i % ff_chunks) * CHUNK, CHUNK), CHUNK)
            inner[i // ff_chunks, :, cols] = (jax.nn.silu(one) * three).astype(jnp.bfloat16)

            @pl.when(g + GU_SLOTS < layers * gu_total)
            def _():
                for c in gu_copies(g + GU_SLOTS):
                    c.start()

            return carry

        lax.fori_loop(0, gu_total, gu_body, 0)

        @pl.when(layer + 1 < layers)
        def _():
            start_attention(layer + 1)

        def near_copies(j):
            return [remote(stage.at[j, pl.ds(toks, toks)], part_l.at[layer, j], ps.at[j], pr.at[layer, j], "ep", partner),
                    remote(stage.at[j, pl.ds(3 * toks, toks)], part_m.at[layer, j], ms.at[j], mr.at[layer, j], "ep", partner)]

        def far_copy(j):
            return remote(merged.at[j], far.at[layer, j], fs.at[j], fr.at[layer, j], "ep", cross)

        def merge(j):
            near_copies(j)[1].wait_recv()
            merged[j] = stage[j, pl.ds(2 * toks, toks), :] + part_m[layer, j]
            far_copy(j).start()

        def d_body(j, carry):
            for k in range(local):
                d = layer * d_total + j * local + k
                slot = d % DOWN_SLOTS
                d_copy(d).wait()
                y = jnp.dot(inner[k], dbuf[slot], preferred_element_type=jnp.float32).astype(jnp.bfloat16).astype(jnp.float32)
                gate = gsel[k]
                for n in range(CHUNK // LANES):
                    cols = slice(n * LANES, (n + 1) * LANES)
                    term = jnp.where(gate > 0.0, gate * y[:, cols], 0.0)
                    if k > 0:
                        term = stage[j, :, cols] + term
                    stage[j, :, cols] = term

                @pl.when(d + DOWN_SLOTS < layers * d_total)
                def _():
                    d_copy(d + DOWN_SLOTS).start()

            for c in reversed(near_copies(j)):
                c.start()

            @pl.when(j > 0)
            def _():
                merge(j - 1)

            return carry

        lax.fori_loop(0, d_chunks, d_body, 0)
        merge(d_chunks - 1)

        for j in range(d_chunks):
            cols = slice(j * CHUNK, (j + 1) * CHUNK)
            near_copies(j)[0].wait_recv()
            far_copy(j).wait_recv()
            total = (stage[j, pl.ds(0, toks), :] + part_l[layer, j]) + far[layer, j]
            acc_a[:, cols] = (acc_a[:, cols].astype(jnp.float32) + total).astype(jnp.bfloat16)

        for c in (u_near, u_far, u_pass, g_near, g_far, g_pass):
            c.wait_send()
        for j in range(d_chunks):
            for c in near_copies(j):
                c.wait_send()
            far_copy(j).wait_send()
        return carry

    lax.fori_loop(0, layers, layer_body, 0)

    xg[p] = acc_a[...]

    def shift(origin, way):
        return remote(xg.at[origin], xg.at[origin], zs.at[way, origin], zr.at[origin], "pool", p + 1 - 2 * way)

    def store(origin):
        return pltpu.make_async_copy(xg.at[origin], out.at[pl.ds(origin * toks, toks)], osem.at[origin])

    @pl.when(p < pools - 1)
    def _():
        shift(p, 0).start()

    @pl.when(p > 0)
    def _():
        shift(p, 1).start()

    store(p).start()
    for step in range(1, pools):
        @pl.when(p - step >= 0)
        def _(step=step):
            shift(p - step, 0).wait_recv()

            @pl.when(p < pools - 1)
            def _():
                shift(p - step, 0).start()

            store(p - step).start()

        @pl.when(p + step < pools)
        def _(step=step):
            shift(p + step, 1).wait_recv()

            @pl.when(p > 0)
            def _():
                shift(p + step, 1).start()

            store(p + step).start()

    for step in range(pools):
        @pl.when((p - step >= 0) & (p < pools - 1))
        def _(step=step):
            shift(p - step, 0).wait_send()

        @pl.when((p + step < pools) & (p > 0))
        def _(step=step):
            shift(p + step, 1).wait_send()

    for origin in range(pools):
        store(origin).wait()


def solution(mesh):
    pools = mesh.shape["pool"]

    def body(hidden, k_cache, v_cache, lengths, expert_ids, w_query, w_key, w_value, w_out, w_router, w_gate, w_up, w_down):
        layers, shard, seq, kv_heads, head = k_cache.shape
        model = hidden.shape[1]
        toks = shard // pools
        local, ff = w_gate.shape[1], w_gate.shape[3]
        heads = w_query.shape[2] // head
        dims = (layers, toks, model, ff, heads, local)
        cos_t, sin_t = rotary_tables(seq + 8)
        f32, bf16 = jnp.float32, jnp.bfloat16
        d_chunks = model // CHUNK
        dma, vmem = pltpu.SemaphoreType.DMA, pltpu.VMEM
        scratch = [
            vmem((model, heads * head), bf16), vmem((model, 2 * kv_heads * head), bf16), vmem((heads * head, model), bf16),
            vmem((toks, seq * kv_heads, head), bf16), vmem((toks, seq * kv_heads, head), bf16),
            vmem((GU_SLOTS, 2, model, CHUNK), bf16), vmem((DOWN_SLOTS, ff, CHUNK), bf16),
            vmem((layers, 4 * toks, model), bf16), vmem((local, 4 * toks, ff), bf16),
            vmem((d_chunks, 4 * toks, CHUNK), f32),
            vmem((layers, d_chunks, toks, CHUNK), f32), vmem((layers, d_chunks, toks, CHUNK), f32),
            vmem((d_chunks, toks, CHUNK), f32), vmem((layers, d_chunks, toks, CHUNK), f32),
            vmem((pools, toks, model), bf16), vmem((toks, model), bf16),
            vmem((16 * toks, head), f32), vmem((16 * toks, head), f32), vmem((16 * toks, head), f32), vmem((16 * toks, head), f32),
            vmem((toks, heads * head), bf16), vmem((layers, 4 * toks, LANES), f32), vmem((local, 4 * toks, LANES), f32),
            vmem((layers, w_router.shape[2], model), f32),
            vmem(cos_t.shape, f32), vmem(sin_t.shape, f32), vmem((toks, head), f32), vmem((toks, head), f32),
            vmem((layers, 2, toks, LANES), jnp.int32),
            dma((4,)), dma((KV_BLOCKS, 2)), dma((GU_SLOTS, 2)), dma((DOWN_SLOTS,)), dma((4,)),
            dma((3,)), dma((layers, 3)), dma((3,)), dma((layers, 3)),
            dma((d_chunks,)), dma((layers, d_chunks)), dma((d_chunks,)), dma((layers, d_chunks)),
            dma((d_chunks,)), dma((layers, d_chunks)), dma((2, pools)), dma((pools,)), dma((pools,)),
        ]
        smem = pl.BlockSpec(memory_space=pltpu.SMEM)
        anyw = pl.BlockSpec(memory_space=pl.ANY)
        return pl.pallas_call(
            functools.partial(kernel, dims),
            out_shape=jax.ShapeDtypeStruct((shard, model), bf16),
            in_specs=[smem, smem] + [anyw] * 13,
            out_specs=anyw,
            scratch_shapes=scratch,
            compiler_params=pltpu.CompilerParams(collective_id=0, has_side_effects=True, vmem_limit_bytes=67043328),
            name="decode",
        )(lengths, jnp.swapaxes(expert_ids, 1, 2), hidden,
          k_cache.reshape(layers, shard, seq * kv_heads, head), v_cache.reshape(layers, shard, seq * kv_heads, head),
          w_query, w_key, w_value, w_out, jnp.swapaxes(w_router, 1, 2), jnp.asarray(cos_t), jnp.asarray(sin_t),
          w_gate, w_up, w_down)

    rows_spec = ("dp", "ep")
    in_specs = (P(rows_spec, None), P(None, rows_spec), P(None, rows_spec), P(rows_spec), P(None, rows_spec, None), P(), P(), P(), P(), P(), P(None, "ep"), P(None, "ep"), P(None, "ep"))
    return jax.shard_map(body, mesh=mesh, in_specs=in_specs, out_specs=P(rows_spec, None), check_vma=False)
```

```python
import functools
import math

import jax
import jax.numpy as jnp
import numpy as np
from jax import lax
from jax.experimental import pallas as pl
from jax.experimental.pallas import tpu as pltpu
from jax.sharding import PartitionSpec as P

EPSILON = 1e-6
ROPE_BASE = 10000.0
MESH = pl.DeviceIdType.MESH
HEAD = 128
KV = 2
LANES = 128
CHUNK = 512
GU_SLOTS = 5
DOWN_SLOTS = 3
DOWN_COLS = 256
KV_BLOCKS = 4
GROUP = 8
LAG = 4


def rotary_tables(size):
    half = HEAD // 2
    freqs = np.float32(ROPE_BASE) ** (np.float32(-2.0) * np.arange(half, dtype=np.float32) / np.float32(HEAD))
    angle = np.arange(size, dtype=np.float32)[:, None] * freqs[None, :].astype(np.float32)
    cosine = np.cos(angle).astype(np.float32)
    sine = np.sin(angle).astype(np.float32)
    return np.concatenate([cosine, cosine], 1), np.concatenate([-sine, sine], 1)


def normed(values):
    return values * lax.rsqrt(jnp.mean(values * values, axis=-1, keepdims=True) + EPSILON)


def kernel(dims, lens, ids, hid, kc, vc, wq, wk, wv, wo, wr, cos_t, sin_t, wg, wu, wd, out,
           wq_b, wkv_b, wo_b, kbuf, vbuf, gu, dbuf, ubuf, inner, stage, part_l, part_m, merged, far, xg, acc_a,
           q2d, k2d, v2d, o2d, s_even, s_odd, att, gbuf, gsel, wr_b, cosb, sinb, cosr, sinr, id_b,
           wsem, kvsem, gusem, dsem, isem, us, ur, gs, gr, ps, pr, ms, mr, fs, fr, zs, zr, osem):
    layers, toks, model, ff, heads, local = dims
    e = lax.axis_index("ep")
    p = lax.axis_index("pool")
    pools = 4
    partner = e + 1 - 2 * (e % 2)
    cross = (e + 2) % 4
    start = p * toks
    ff_chunks = ff // CHUNK
    gu_total = local * ff_chunks
    d_chunks = model // DOWN_COLS
    rows = 4 * toks
    half = toks // 2
    group = heads // KV
    seq2 = kbuf.shape[1]
    per_block = toks // KV_BLOCKS

    def remote(src, dst, ssem, rsem, axis, index):
        return pltpu.make_async_remote_copy(src_ref=src, dst_ref=dst, send_sem=ssem, recv_sem=rsem,
                                            device_id={axis: index}, device_id_type=MESH)

    def columns(j):
        return pl.ds(pl.multiple_of(j * DOWN_COLS, DOWN_COLS), DOWN_COLS)

    def gu_copies(g):
        layer, i, slot = g // gu_total, g % gu_total, g % GU_SLOTS
        expert, c = i // ff_chunks, i % ff_chunks
        cols = pl.ds(pl.multiple_of(c * CHUNK, CHUNK), CHUNK)
        return [pltpu.make_async_copy(w.at[layer, expert, :, cols], gu.at[slot, k], gusem.at[slot, k])
                for k, w in enumerate((wg, wu))]

    def d_copies(d):
        layer, j, slot = d // d_chunks, d % d_chunks, d % DOWN_SLOTS
        return [pltpu.make_async_copy(wd.at[layer, k, :, columns(j)], dbuf.at[slot, k], dsem.at[slot, k]) for k in range(local)]

    kvw = KV * HEAD

    def weight_copies(layer):
        return [pltpu.make_async_copy(wq.at[layer], wq_b, wsem.at[0]),
                pltpu.make_async_copy(wk.at[layer], wkv_b.at[:, pl.ds(0, kvw)], wsem.at[1]),
                pltpu.make_async_copy(wv.at[layer], wkv_b.at[:, pl.ds(kvw, kvw)], wsem.at[2]),
                pltpu.make_async_copy(wo.at[layer], wo_b, wsem.at[3])]

    def kv_copies(layer, b):
        here = pl.ds(start + b * per_block, per_block)
        there = pl.ds(b * per_block, per_block)
        return [pltpu.make_async_copy(kc.at[layer, here], kbuf.at[there], kvsem.at[b, 0]),
                pltpu.make_async_copy(vc.at[layer, here], vbuf.at[there], kvsem.at[b, 1])]

    def start_attention(layer):
        copies = weight_copies(layer)
        for c in copies[:3]:
            c.start()
        for b in range(KV_BLOCKS):
            for c in kv_copies(layer, b):
                c.start()
        copies[3].start()

    first = [pltpu.make_async_copy(hid.at[pl.ds(start, toks)], acc_a, isem.at[0]),
             pltpu.make_async_copy(wr, wr_b, isem.at[1]),
             pltpu.make_async_copy(cos_t, cosb, isem.at[2]),
             pltpu.make_async_copy(sin_t, sinb, isem.at[3])]
    for c in first:
        c.start()
    start_attention(0)

    barrier = pltpu.get_barrier_semaphore()
    pl.semaphore_signal(barrier, inc=1, device_id={"ep": partner}, device_id_type=MESH)
    pl.semaphore_signal(barrier, inc=1, device_id={"ep": cross}, device_id_type=MESH)

    @pl.when(p > 0)
    def _():
        pl.semaphore_signal(barrier, inc=1, device_id={"pool": p - 1}, device_id_type=MESH)

    @pl.when(p < pools - 1)
    def _():
        pl.semaphore_signal(barrier, inc=1, device_id={"pool": p + 1}, device_id_type=MESH)

    middle = (p > 0) & (p < pools - 1)

    @pl.when(middle)
    def _():
        pl.semaphore_wait(barrier, 4)

    @pl.when(jnp.logical_not(middle))
    def _():
        pl.semaphore_wait(barrier, 3)

    for c in first:
        c.wait()

    zeros = jnp.zeros(((16 - heads) * toks, HEAD), jnp.float32)
    for ref in (q2d, k2d, v2d):
        ref[pl.ds(heads * toks, (16 - heads) * toks), :] = zeros

    def spread(t, carry):
        where = pl.ds(t, 1)
        n = lens[start + t]
        cosr[where, :] = cosb[pl.ds(n, 1), :]
        sinr[where, :] = sinb[pl.ds(n, 1), :]
        for layer in range(layers):
            for k in range(2):
                id_b[layer, k, where, :] = jnp.full((1, LANES), ids[layer, k, start + t], jnp.int32)
        return carry

    lax.fori_loop(0, toks, spread, 0)

    lane = lax.broadcasted_iota(jnp.int32, (16, seq2), 1)
    head_kv = jnp.where(lax.broadcasted_iota(jnp.int32, (16, seq2), 0) >= group, 1, 0)
    parity = (lane % KV) == head_kv
    scale = HEAD ** -0.5

    def layer_body(layer, carry):
        hidden = acc_a[...].astype(jnp.float32)
        h = normed(hidden).astype(jnp.bfloat16)
        copies = weight_copies(layer)
        copies[0].wait()
        cosine, sine = cosr[...], sinr[...]

        def rope(v):
            return (v * cosine + pltpu.roll(v, HEAD // 2, 1) * sine).astype(jnp.bfloat16).astype(jnp.float32)

        for n in range(heads * HEAD // CHUNK):
            qn = jnp.dot(h, wq_b[:, n * CHUNK:(n + 1) * CHUNK], preferred_element_type=jnp.float32)
            for k in range(CHUNK // HEAD):
                head = n * (CHUNK // HEAD) + k
                q2d[pl.ds(head * toks, toks), :] = rope(qn[:, k * HEAD:(k + 1) * HEAD])
        copies[1].wait()
        copies[2].wait()
        kv = jnp.dot(h, wkv_b[...], preferred_element_type=jnp.float32)
        for j in range(KV):
            kj = rope(kv[:, j * HEAD:(j + 1) * HEAD])
            vj = kv[:, kvw + j * HEAD:kvw + (j + 1) * HEAD].astype(jnp.bfloat16).astype(jnp.float32)
            for k in range(group):
                at = pl.ds((j * group + k) * toks, toks)
                k2d[at, :] = kj
                v2d[at, :] = vj

        @pl.when(layer == 0)
        def _():
            for g in range(GU_SLOTS):
                for c in gu_copies(g):
                    c.start()

        def score(first_token, ref):
            for k in range(GROUP):
                q = q2d[pl.ds(first_token + k, 16, stride=toks), :].astype(jnp.bfloat16)
                ref[k * 16:(k + 1) * 16, :] = lax.dot_general(q, kbuf[first_token + k], (((1,), (1,)), ((), ())),
                                                              preferred_element_type=jnp.float32)

        def mix(first_token, ref):
            weights, news, totals = [], [], []
            for k in range(GROUP):
                at = pl.ds(first_token + k, 16, stride=toks)
                n2 = lens[start + first_token + k] * KV
                s = jnp.where(parity & (lane < n2), ref[k * 16:(k + 1) * 16, :] * scale, -jnp.inf)
                s_new = jnp.sum(q2d[at, :] * k2d[at, :], axis=1, keepdims=True) * scale
                peak = jnp.maximum(jnp.max(s, axis=1, keepdims=True), s_new)
                w = jnp.exp(s - peak)
                w_new = jnp.exp(s_new - peak)
                totals.append(jnp.sum(w, axis=1, keepdims=True) + w_new)
                weights.append(w.astype(jnp.bfloat16))
                news.append(w_new.astype(jnp.bfloat16).astype(jnp.float32))
            sums = [jnp.dot(weights[k], vbuf[first_token + k], preferred_element_type=jnp.float32) for k in range(GROUP)]
            for k in range(GROUP):
                at = pl.ds(first_token + k, 16, stride=toks)
                o2d[at, :] = (sums[k] + news[k] * v2d[at, :]) / totals[k]

        kv_copies(layer, 0)[0].wait()
        score(0, s_even)

        def attend(i, carry):
            kv_copies(layer, i)[1].wait()

            @pl.when(i + 1 < KV_BLOCKS)
            def _():
                kv_copies(layer, i + 1)[0].wait()

            t = i * per_block
            score(t + GROUP, s_odd)
            mix(t, s_even)
            score((t + 2 * GROUP) % toks, s_even)
            mix(t + GROUP, s_odd)
            return carry

        lax.fori_loop(0, KV_BLOCKS, attend, 0)

        @pl.when(layer == 0)
        def _():
            for d in range(DOWN_SLOTS):
                for c in d_copies(d):
                    c.start()

        for head in range(heads):
            att[:, head * HEAD:(head + 1) * HEAD] = o2d[pl.ds(head * toks, toks), :].astype(jnp.bfloat16)
        copies[3].wait()
        for n in range(model // CHUNK):
            cols = slice(n * CHUNK, (n + 1) * CHUNK)
            a = acc_a[:, cols].astype(jnp.float32) + jnp.dot(att[...], wo_b[:, cols], preferred_element_type=jnp.float32)
            acc_a[:, cols] = a.astype(jnp.bfloat16)

        u = normed(acc_a[...].astype(jnp.float32)).astype(jnp.bfloat16)
        ubuf[layer, pl.ds(0, toks), :] = u

        def block(ref, b):
            return ref.at[layer, pl.ds(b * toks, toks)]

        def piece(b, h):
            return ubuf.at[layer, pl.ds(b * toks + h * half, half)]

        u_near = [remote(piece(0, h), piece(1, h), us.at[0, h], ur.at[layer, 0, h], "ep", partner) for h in range(2)]
        u_far = [remote(piece(0, h), piece(2, h), us.at[1, h], ur.at[layer, 1, h], "ep", cross) for h in range(2)]
        u_pass = [remote(piece(2, h), piece(3, h), us.at[2, h], ur.at[layer, 2, h], "ep", partner) for h in range(2)]
        g_near = remote(block(gbuf, 0), block(gbuf, 1), gs.at[0], gr.at[layer, 0], "ep", partner)
        g_far = remote(block(gbuf, 0), block(gbuf, 2), gs.at[1], gr.at[layer, 1], "ep", cross)
        g_pass = remote(block(gbuf, 2), block(gbuf, 3), gs.at[2], gr.at[layer, 2], "ep", partner)
        for c in u_far + u_near:
            c.start()

        wl = wr_b[layer]
        hi = wl.astype(jnp.bfloat16).astype(jnp.float32)
        rest = wl - hi
        mid = rest.astype(jnp.bfloat16).astype(jnp.float32)
        low = rest - mid
        wide = jnp.concatenate([hi, mid, low, jnp.zeros((LANES - 3 * wl.shape[0], model), jnp.float32)], axis=0).astype(jnp.bfloat16)
        parts = lax.dot_general(u, wide, (((1,), (1,)), ((), ())), preferred_element_type=jnp.float32)
        logits = parts + pltpu.roll(parts, LANES - 8, 1) + pltpu.roll(parts, LANES - 16, 1)
        expert_lane = lax.broadcasted_iota(jnp.int32, (toks, LANES), 1)
        chosen = (id_b[layer, 0] == expert_lane) | (id_b[layer, 1] == expert_lane)
        logits = jnp.where(chosen, logits, -jnp.inf)
        ew = jnp.exp(logits - jnp.max(logits, axis=1, keepdims=True))
        gbuf[layer, pl.ds(0, toks), :] = ew / jnp.sum(ew, axis=1, keepdims=True)
        g_far.start()
        g_near.start()

        def gate_up(low, count, wait, release):
            def step(i, carry):
                g = layer * gu_total + i
                slot = g % GU_SLOTS
                if wait:
                    for c in gu_copies(g):
                        c.wait()
                tokens = ubuf[layer, low:low + count, :]
                one = jnp.dot(tokens, gu[slot, 0], preferred_element_type=jnp.float32)
                three = jnp.dot(tokens, gu[slot, 1], preferred_element_type=jnp.float32)
                cols = pl.ds(pl.multiple_of((i % ff_chunks) * CHUNK, CHUNK), CHUNK)
                inner[i // ff_chunks, low:low + count, cols] = (jax.nn.silu(one) * three).astype(jnp.bfloat16)
                if release:
                    @pl.when(g + GU_SLOTS < layers * gu_total)
                    def _():
                        for c in gu_copies(g + GU_SLOTS):
                            c.start()

                return carry

            return step

        for c in u_near:
            c.wait_recv()
        lax.fori_loop(0, 3, gate_up(0, 2 * toks, True, False), 0)
        u_far[0].wait_recv()
        u_pass[0].start()
        lax.fori_loop(3, GU_SLOTS, gate_up(0, 2 * toks, True, False), 0)
        u_far[1].wait_recv()
        u_pass[1].start()
        g_far.wait_recv()
        g_pass.start()
        for c in u_pass:
            c.wait_recv()
        lax.fori_loop(0, GU_SLOTS, gate_up(2 * toks, 2 * toks, False, True), 0)
        lax.fori_loop(GU_SLOTS, gu_total, gate_up(0, 4 * toks, True, True), 0)

        g_near.wait_recv()
        g_pass.wait_recv()
        gates = gbuf[layer]
        row_lane = lax.broadcasted_iota(jnp.int32, (rows, LANES), 1)
        for k in range(local):
            one = jnp.sum(jnp.where(row_lane == e * local + k, gates, 0.0), axis=1, keepdims=True)
            gsel[k] = jnp.broadcast_to(one, (rows, LANES))

        @pl.when(layer + 1 < layers)
        def _():
            start_attention(layer + 1)

        def near_l(j):
            return remote(stage.at[j, pl.ds(toks, toks)], part_l.at[layer, j], ps.at[j], pr.at[layer, j], "ep", partner)

        def near_m(j):
            return remote(stage.at[j, pl.ds(3 * toks, toks)], part_m.at[layer, j], ms.at[j], mr.at[layer, j], "ep", partner)

        def far_copy(j):
            return remote(merged.at[j], far.at[layer, j], fs.at[j], fr.at[layer, j], "ep", cross)

        def merge(j):
            near_m(j).wait_recv()
            merged[j] = stage[j, pl.ds(2 * toks, toks), :] + part_m[layer, j]
            far_copy(j).start()

        def combine(c):
            near_l(c).wait_recv()
            far_copy(c).wait_recv()
            total = (stage[c, pl.ds(0, toks), :] + part_l[layer, c]) + far[layer, c]
            x = (acc_a[:, columns(c)].astype(jnp.float32) + total).astype(jnp.bfloat16)
            acc_a[:, columns(c)] = x

            @pl.when(layer == layers - 1)
            def _():
                xg[p, :, columns(c)] = x
                store(p, c).start()

                @pl.when(p < pools - 1)
                def _():
                    shift(p, c, 0).start()

                @pl.when(p > 0)
                def _():
                    shift(p, c, 1).start()

        def down(j, slot, low):
            terms = [None] * (DOWN_COLS // LANES)
            for k in range(local):
                y = jnp.dot(inner[k, low:low + 2 * toks, :], dbuf[slot, k], preferred_element_type=jnp.float32)
                y = y.astype(jnp.bfloat16).astype(jnp.float32)
                gate = gsel[k, low:low + 2 * toks, :]
                for n in range(len(terms)):
                    term = jnp.where(gate > 0.0, gate * y[:, n * LANES:(n + 1) * LANES], 0.0)
                    terms[n] = term if k == 0 else terms[n] + term
            for n in range(len(terms)):
                stage[j, low:low + 2 * toks, n * LANES:(n + 1) * LANES] = terms[n]

        def down_body(j, carry):
            d = layer * d_chunks + j
            slot = d % DOWN_SLOTS
            for c in d_copies(d):
                c.wait()
            down(j, slot, 2 * toks)
            near_m(j).start()

            @pl.when(j > 0)
            def _():
                merge(j - 1)

            down(j, slot, 0)
            near_l(j).start()

            @pl.when(d + DOWN_SLOTS < layers * d_chunks)
            def _():
                for c in d_copies(d + DOWN_SLOTS):
                    c.start()

            @pl.when(j >= LAG)
            def _():
                combine(j - LAG)

            return carry

        lax.fori_loop(0, d_chunks, down_body, 0)
        merge(d_chunks - 1)

        def last_ones(c, carry):
            combine(c)
            return carry

        lax.fori_loop(d_chunks - LAG, d_chunks, last_ones, 0)

        for c in u_near + u_far + u_pass + [g_near, g_far, g_pass]:
            c.wait_send()

        def sent(j, carry):
            near_l(j).wait_send()
            near_m(j).wait_send()
            far_copy(j).wait_send()
            return carry

        lax.fori_loop(0, d_chunks, sent, 0)
        return carry

    def shift(origin, c, way):
        at = xg.at[origin, :, columns(c)]
        return remote(at, at, zs.at[way, origin, c], zr.at[origin, c], "pool", p + 1 - 2 * way)

    def store(origin, c):
        here = pl.ds(origin * toks, toks)
        return pltpu.make_async_copy(xg.at[origin, :, columns(c)], out.at[here, columns(c)], osem.at[origin, c])

    lax.fori_loop(0, layers, layer_body, 0)

    def wave(i, carry):
        for step in range(1, pools):
            c = i - (step - 1)
            live = (c >= 0) & (c < d_chunks)

            @pl.when(live & (p - step >= 0))
            def _(step=step, c=c):
                shift(p - step, c, 0).wait_recv()

                @pl.when(p < pools - 1)
                def _():
                    shift(p - step, c, 0).start()

                store(p - step, c).start()

            @pl.when(live & (p + step < pools))
            def _(step=step, c=c):
                shift(p + step, c, 1).wait_recv()

                @pl.when(p > 0)
                def _():
                    shift(p + step, c, 1).start()

                store(p + step, c).start()

        return carry

    lax.fori_loop(0, d_chunks + pools - 2, wave, 0)

    def finish(c, carry):
        for step in range(pools):
            @pl.when((p - step >= 0) & (p < pools - 1))
            def _(step=step):
                shift(p - step, c, 0).wait_send()

            @pl.when((p + step < pools) & (p > 0))
            def _(step=step):
                shift(p + step, c, 1).wait_send()

        for origin in range(pools):
            store(origin, c).wait()
        return carry

    lax.fori_loop(0, d_chunks, finish, 0)


def solution(mesh):
    pools = mesh.shape["pool"]

    def body(hidden, k_cache, v_cache, lengths, expert_ids, w_query, w_key, w_value, w_out, w_router, w_gate, w_up, w_down):
        layers, shard, seq, kv_heads, head = k_cache.shape
        model = hidden.shape[1]
        toks = shard // pools
        local, ff = w_gate.shape[1], w_gate.shape[3]
        heads = w_query.shape[2] // head
        dims = (layers, toks, model, ff, heads, local)
        cos_t, sin_t = rotary_tables(seq + 8)
        f32, bf16 = jnp.float32, jnp.bfloat16
        d_chunks = model // DOWN_COLS
        dma, vmem = pltpu.SemaphoreType.DMA, pltpu.VMEM
        scratch = [
            vmem((model, heads * head), bf16), vmem((model, 2 * kv_heads * head), bf16), vmem((heads * head, model), bf16),
            vmem((toks, seq * kv_heads, head), bf16), vmem((toks, seq * kv_heads, head), bf16),
            vmem((GU_SLOTS, 2, model, CHUNK), bf16), vmem((DOWN_SLOTS, local, ff, DOWN_COLS), bf16),
            vmem((layers, 4 * toks, model), bf16), vmem((local, 4 * toks, ff), bf16),
            vmem((d_chunks, 4 * toks, DOWN_COLS), f32),
            vmem((layers, d_chunks, toks, DOWN_COLS), f32), vmem((layers, d_chunks, toks, DOWN_COLS), f32),
            vmem((d_chunks, toks, DOWN_COLS), f32), vmem((layers, d_chunks, toks, DOWN_COLS), f32),
            vmem((pools, toks, model), bf16), vmem((toks, model), bf16),
            vmem((16 * toks, head), f32), vmem((16 * toks, head), f32), vmem((16 * toks, head), f32), vmem((16 * toks, head), f32),
            vmem((GROUP * 16, seq * kv_heads), f32), vmem((GROUP * 16, seq * kv_heads), f32),
            vmem((toks, heads * head), bf16), vmem((layers, 4 * toks, LANES), f32), vmem((local, 4 * toks, LANES), f32),
            vmem((layers, w_router.shape[2], model), f32),
            vmem(cos_t.shape, f32), vmem(sin_t.shape, f32), vmem((toks, head), f32), vmem((toks, head), f32),
            vmem((layers, 2, toks, LANES), jnp.int32),
            dma((4,)), dma((KV_BLOCKS, 2)), dma((GU_SLOTS, 2)), dma((DOWN_SLOTS, local)), dma((4,)),
            dma((3, 2)), dma((layers, 3, 2)), dma((3,)), dma((layers, 3)),
            dma((d_chunks,)), dma((layers, d_chunks)), dma((d_chunks,)), dma((layers, d_chunks)),
            dma((d_chunks,)), dma((layers, d_chunks)), dma((2, pools, d_chunks)), dma((pools, d_chunks)), dma((pools, d_chunks)),
        ]
        smem = pl.BlockSpec(memory_space=pltpu.SMEM)
        anyw = pl.BlockSpec(memory_space=pl.ANY)
        return pl.pallas_call(
            functools.partial(kernel, dims),
            out_shape=jax.ShapeDtypeStruct((shard, model), bf16),
            in_specs=[smem, smem] + [anyw] * 13,
            out_specs=anyw,
            scratch_shapes=scratch,
            compiler_params=pltpu.CompilerParams(collective_id=0, has_side_effects=True, vmem_limit_bytes=67043328),
            name="decode",
        )(lengths, jnp.swapaxes(expert_ids, 1, 2), hidden,
          k_cache.reshape(layers, shard, seq * kv_heads, head), v_cache.reshape(layers, shard, seq * kv_heads, head),
          w_query, w_key, w_value, w_out, jnp.swapaxes(w_router, 1, 2), jnp.asarray(cos_t), jnp.asarray(sin_t),
          w_gate, w_up, w_down)

    rows_spec = ("dp", "ep")
    in_specs = (P(rows_spec, None), P(None, rows_spec), P(None, rows_spec), P(rows_spec), P(None, rows_spec, None), P(), P(), P(), P(), P(), P(None, "ep"), P(None, "ep"), P(None, "ep"))
    return jax.shard_map(body, mesh=mesh, in_specs=in_specs, out_specs=P(rows_spec, None), check_vma=False)
```

```python
import functools
import math

import jax
import jax.numpy as jnp
import numpy as np
from jax import lax
from jax.experimental import pallas as pl
from jax.experimental.pallas import tpu as pltpu
from jax.sharding import PartitionSpec as P

EPSILON = 1e-6
ROPE_BASE = 10000.0
MESH = pl.DeviceIdType.MESH
HEAD = 128
KV = 2
LANES = 128
CHUNK = 512
GU_COLS = 1024
GU_SLOTS = 4
PIECE = 256
DOWN_SLOTS = 3
DOWN_COLS = 256
KV_BLOCKS = 4
GROUP = 8
LAG = 4
ATTENTION_AT = 3
WAYS = (-2, 2, -1, 1)
RELAY_LAG = 2


def rotary_tables(size):
    half = HEAD // 2
    freqs = np.float32(ROPE_BASE) ** (np.float32(-2.0) * np.arange(half, dtype=np.float32) / np.float32(HEAD))
    angle = np.arange(size, dtype=np.float32)[:, None] * freqs[None, :].astype(np.float32)
    cosine = np.cos(angle).astype(np.float32)
    sine = np.sin(angle).astype(np.float32)
    return np.concatenate([cosine, cosine], 1), np.concatenate([-sine, sine], 1)


def normed(values):
    return values * lax.rsqrt(jnp.mean(values * values, axis=-1, keepdims=True) + EPSILON)


def kernel(dims, lens, ids, hid, kc, vc, wq, wk, wv, wo, wr, cos_t, sin_t, wg, wu, wd, out,
           wo_b, kbuf, vbuf, gu, dbuf, ubuf, inner, stage, part_l, part_m, merged, far, xg, acc_a,
           q2d, k2d, v2d, o2d, s_even, s_odd, att, gbuf, gsel, wr_b, cosb, sinb, cosr, sinr, id_b,
           wsem, kvsem, gusem, dsem, isem, us, ur, gs, gr, ps, pr, ms, mr, fs, fr, zs, zr, osem):
    layers, toks, model, ff, heads, local = dims
    e = lax.axis_index("ep")
    p = lax.axis_index("pool")
    pools = 4
    partner = e + 1 - 2 * (e % 2)
    cross = (e + 2) % 4
    start = p * toks
    ff_chunks = ff // GU_COLS
    gu_total = local * ff_chunks
    d_chunks = model // DOWN_COLS
    rows = 4 * toks
    half = toks // 2
    group = heads // KV
    seq2 = kbuf.shape[1]
    per_block = toks // KV_BLOCKS

    def remote(src, dst, ssem, rsem, axis, index):
        return pltpu.make_async_remote_copy(src_ref=src, dst_ref=dst, send_sem=ssem, recv_sem=rsem,
                                            device_id={axis: index}, device_id_type=MESH)

    def columns(j):
        return pl.ds(pl.multiple_of(j * DOWN_COLS, DOWN_COLS), DOWN_COLS)

    def gu_copies(g):
        layer, i, slot = g // gu_total, g % gu_total, (g % gu_total) % GU_SLOTS
        expert, c = i // ff_chunks, i % ff_chunks
        cols = pl.ds(pl.multiple_of(c * GU_COLS, GU_COLS), GU_COLS)
        return [pltpu.make_async_copy(w.at[layer, expert, :, cols], gu.at[slot, k], gusem.at[slot, k])
                for k, w in enumerate((wg, wu))]

    def d_copies(d):
        layer, j, slot = d // d_chunks, d % d_chunks, (d % d_chunks) % DOWN_SLOTS
        return [pltpu.make_async_copy(wd.at[layer, k, :, columns(j)], dbuf.at[slot, k], dsem.at[slot, k]) for k in range(local)]

    kvw = KV * HEAD
    q_cols = heads * HEAD

    def proj(column, count):
        return gu.at[GU_SLOTS - 1, column // GU_COLS, :, pl.ds(column % GU_COLS, count)]

    def weight_copies(layer):
        pieces = range(q_cols // CHUNK)
        return [pltpu.make_async_copy(wk.at[layer], proj(q_cols, kvw), wsem.at[0]),
                pltpu.make_async_copy(wv.at[layer], proj(q_cols + kvw, kvw), wsem.at[1]),
                pltpu.make_async_copy(wo.at[layer], wo_b, wsem.at[2]),
                *(pltpu.make_async_copy(wq.at[layer, :, pl.ds(n * CHUNK, CHUNK)], proj(n * CHUNK, CHUNK), wsem.at[3 + n]) for n in pieces)]

    def kv_copies(layer, b):
        here = pl.ds(start + b * per_block, per_block)
        there = pl.ds(b * per_block, per_block)
        return [pltpu.make_async_copy(kc.at[layer, here], kbuf.at[there], kvsem.at[b, 0]),
                pltpu.make_async_copy(vc.at[layer, here], vbuf.at[there], kvsem.at[b, 1])]

    def start_projections(layer):
        copies = weight_copies(layer)
        for c in copies[3:] + copies[:2]:
            c.start()

    def start_caches(layer):
        for b in range(KV_BLOCKS):
            for c in kv_copies(layer, b):
                c.start()
        weight_copies(layer)[2].start()

    def start_attention(layer):
        start_projections(layer)
        start_caches(layer)

    def start_gate_up(layer):
        for i in range(GU_SLOTS - 1):
            for c in gu_copies(layer * gu_total + i):
                c.start()

    def start_down(layer):
        for j in range(DOWN_SLOTS):
            for c in d_copies(layer * d_chunks + j):
                c.start()

    first = [pltpu.make_async_copy(hid.at[pl.ds(start, toks)], acc_a, isem.at[0]),
             pltpu.make_async_copy(wr, wr_b, isem.at[1]),
             pltpu.make_async_copy(cos_t, cosb, isem.at[2]),
             pltpu.make_async_copy(sin_t, sinb, isem.at[3])]
    first[0].start()
    start_projections(0)
    for c in first[1:]:
        c.start()

    barrier = pltpu.get_barrier_semaphore()
    pl.semaphore_signal(barrier, inc=1, device_id={"ep": partner}, device_id_type=MESH)
    pl.semaphore_signal(barrier, inc=1, device_id={"ep": cross}, device_id_type=MESH)

    inside = (p > 0) & (p < pools - 1)
    for way in (-2, -1, 1, 2):
        @pl.when((p + way >= 0) & (p + way < pools))
        def _(way=way):
            pl.semaphore_signal(barrier, inc=1, device_id={"pool": p + way}, device_id_type=MESH)

    for c in first:
        c.wait()

    zeros = jnp.zeros(((16 - heads) * toks, HEAD), jnp.float32)
    for ref in (q2d, k2d, v2d):
        ref[pl.ds(heads * toks, (16 - heads) * toks), :] = zeros

    def spread(t, carry):
        where = pl.ds(t, 1)
        n = lens[start + t]
        cosr[where, :] = cosb[pl.ds(n, 1), :]
        sinr[where, :] = sinb[pl.ds(n, 1), :]
        for layer in range(layers):
            for k in range(2):
                id_b[layer, k, where, :] = jnp.full((1, LANES), ids[layer, k, start + t], jnp.int32)
        return carry

    lax.fori_loop(0, toks, spread, 0)
    start_caches(0)

    lane = lax.broadcasted_iota(jnp.int32, (16, seq2), 1)
    head_kv = jnp.where(lax.broadcasted_iota(jnp.int32, (16, seq2), 0) >= group, 1, 0)
    parity = (lane % KV) == head_kv
    scale = HEAD ** -0.5

    def layer_body(layer, carry):
        hidden = acc_a[...].astype(jnp.float32)
        h = normed(hidden).astype(jnp.bfloat16)
        copies = weight_copies(layer)
        cosine, sine = cosr[...], sinr[...]

        def rope(v):
            return (v * cosine + pltpu.roll(v, HEAD // 2, 1) * sine).astype(jnp.bfloat16).astype(jnp.float32)

        for n in range(heads * HEAD // CHUNK):
            copies[3 + n].wait()
            qn = jnp.dot(h, proj(n * CHUNK, CHUNK)[...], preferred_element_type=jnp.float32)
            for k in range(CHUNK // HEAD):
                head = n * (CHUNK // HEAD) + k
                q2d[pl.ds(head * toks, toks), :] = rope(qn[:, k * HEAD:(k + 1) * HEAD])
        copies[0].wait()
        copies[1].wait()
        kv = jnp.dot(h, proj(q_cols, 2 * kvw)[...], preferred_element_type=jnp.float32)
        for j in range(KV):
            kj = rope(kv[:, j * HEAD:(j + 1) * HEAD])
            vj = kv[:, kvw + j * HEAD:kvw + (j + 1) * HEAD].astype(jnp.bfloat16).astype(jnp.float32)
            for k in range(group):
                at = pl.ds((j * group + k) * toks, toks)
                k2d[at, :] = kj
                v2d[at, :] = vj

        @pl.when(layer == 0)
        def _():
            start_gate_up(0)

        for c in gu_copies(layer * gu_total + GU_SLOTS - 1):
            c.start()

        def score(first_token, ref):
            for k in range(GROUP):
                q = q2d[pl.ds(first_token + k, 16, stride=toks), :].astype(jnp.bfloat16)
                ref[k * 16:(k + 1) * 16, :] = lax.dot_general(q, kbuf[first_token + k], (((1,), (1,)), ((), ())),
                                                              preferred_element_type=jnp.float32)

        def mix(first_token, ref):
            weights, news, totals = [], [], []
            for k in range(GROUP):
                at = pl.ds(first_token + k, 16, stride=toks)
                n2 = lens[start + first_token + k] * KV
                s = jnp.where(parity & (lane < n2), ref[k * 16:(k + 1) * 16, :] * scale, -jnp.inf)
                s_new = jnp.sum(q2d[at, :] * k2d[at, :], axis=1, keepdims=True) * scale
                peak = jnp.maximum(jnp.max(s, axis=1, keepdims=True), s_new)
                w = jnp.exp(s - peak)
                w_new = jnp.exp(s_new - peak)
                totals.append(jnp.sum(w, axis=1, keepdims=True) + w_new)
                weights.append(w.astype(jnp.bfloat16))
                news.append(w_new.astype(jnp.bfloat16).astype(jnp.float32))
            sums = [jnp.dot(weights[k], vbuf[first_token + k], preferred_element_type=jnp.float32) for k in range(GROUP)]
            for k in range(GROUP):
                at = pl.ds(first_token + k, 16, stride=toks)
                o2d[at, :] = (sums[k] + news[k] * v2d[at, :]) / totals[k]

        kv_copies(layer, 0)[0].wait()
        score(0, s_even)

        def attend(i, carry):
            kv_copies(layer, i)[1].wait()

            @pl.when(i + 1 < KV_BLOCKS)
            def _():
                kv_copies(layer, i + 1)[0].wait()

            t = i * per_block
            score(t + GROUP, s_odd)
            mix(t, s_even)
            score((t + 2 * GROUP) % toks, s_even)
            mix(t + GROUP, s_odd)
            return carry

        lax.fori_loop(0, KV_BLOCKS, attend, 0)

        @pl.when(layer == 0)
        def _():
            start_down(0)

        for head in range(heads):
            att[:, head * HEAD:(head + 1) * HEAD] = o2d[pl.ds(head * toks, toks), :].astype(jnp.bfloat16)
        copies[2].wait()
        for n in range(model // CHUNK):
            cols = slice(n * CHUNK, (n + 1) * CHUNK)
            a = acc_a[:, cols].astype(jnp.float32) + jnp.dot(att[...], wo_b[:, cols], preferred_element_type=jnp.float32)
            acc_a[:, cols] = a.astype(jnp.bfloat16)

        u = normed(acc_a[...].astype(jnp.float32)).astype(jnp.bfloat16)
        ubuf[layer, pl.ds(0, toks), :] = u

        def block(ref, b):
            return ref.at[layer, pl.ds(b * toks, toks)]

        def piece(b, h):
            return ubuf.at[layer, pl.ds(b * toks + h * half, half)]

        u_near = [remote(piece(0, h), piece(1, h), us.at[0, h], ur.at[layer, 0, h], "ep", partner) for h in range(2)]
        u_far = [remote(piece(0, h), piece(2, h), us.at[1, h], ur.at[layer, 1, h], "ep", cross) for h in range(2)]
        u_pass = [remote(piece(2, h), piece(3, h), us.at[2, h], ur.at[layer, 2, h], "ep", partner) for h in range(2)]
        g_near = remote(block(gbuf, 0), block(gbuf, 1), gs.at[0], gr.at[layer, 0], "ep", partner)
        g_far = remote(block(gbuf, 0), block(gbuf, 2), gs.at[1], gr.at[layer, 1], "ep", cross)
        g_pass = remote(block(gbuf, 2), block(gbuf, 3), gs.at[2], gr.at[layer, 2], "ep", partner)
        @pl.when((layer == 0) & inside)
        def _():
            pl.semaphore_wait(barrier, 5)

        @pl.when((layer == 0) & jnp.logical_not(inside))
        def _():
            pl.semaphore_wait(barrier, 4)

        for c in u_far + u_near:
            c.start()

        wl = wr_b[layer]
        hi = wl.astype(jnp.bfloat16).astype(jnp.float32)
        rest = wl - hi
        mid = rest.astype(jnp.bfloat16).astype(jnp.float32)
        low = rest - mid
        wide = jnp.concatenate([hi, mid, low, jnp.zeros((LANES - 3 * wl.shape[0], model), jnp.float32)], axis=0).astype(jnp.bfloat16)
        parts = lax.dot_general(u, wide, (((1,), (1,)), ((), ())), preferred_element_type=jnp.float32)
        logits = parts + pltpu.roll(parts, LANES - 8, 1) + pltpu.roll(parts, LANES - 16, 1)
        expert_lane = lax.broadcasted_iota(jnp.int32, (toks, LANES), 1)
        chosen = (id_b[layer, 0] == expert_lane) | (id_b[layer, 1] == expert_lane)
        logits = jnp.where(chosen, logits, -jnp.inf)
        ew = jnp.exp(logits - jnp.max(logits, axis=1, keepdims=True))
        gbuf[layer, pl.ds(0, toks), :] = ew / jnp.sum(ew, axis=1, keepdims=True)
        g_far.start()
        g_near.start()

        def gate_up(low, count, wait, release):
            def step(i, carry):
                g = layer * gu_total + i
                slot = i % GU_SLOTS
                if wait:
                    for c in gu_copies(g):
                        c.wait()
                for n in range(0, GU_COLS, PIECE):
                    tokens = ubuf[layer, low:low + count, :]
                    one = jnp.dot(tokens, gu[slot, 0, :, n:n + PIECE], preferred_element_type=jnp.float32)
                    three = jnp.dot(tokens, gu[slot, 1, :, n:n + PIECE], preferred_element_type=jnp.float32)
                    cols = pl.ds(pl.multiple_of((i % ff_chunks) * GU_COLS + n, PIECE), PIECE)
                    inner[i // ff_chunks, low:low + count, cols] = (jax.nn.silu(one) * three).astype(jnp.bfloat16)
                if release:
                    @pl.when(i + GU_SLOTS < gu_total)
                    def _():
                        for c in gu_copies(g + GU_SLOTS):
                            c.start()

                return carry

            return step

        for c in u_near:
            c.wait_recv()
        lax.fori_loop(0, 2, gate_up(0, 2 * toks, True, False), 0)
        u_far[0].wait_recv()
        u_pass[0].start()
        lax.fori_loop(2, GU_SLOTS, gate_up(0, 2 * toks, True, False), 0)
        u_far[1].wait_recv()
        u_pass[1].start()
        g_far.wait_recv()
        g_pass.start()
        for c in u_pass:
            c.wait_recv()
        lax.fori_loop(0, GU_SLOTS, gate_up(2 * toks, 2 * toks, False, True), 0)
        lax.fori_loop(GU_SLOTS, gu_total, gate_up(0, 4 * toks, True, True), 0)

        g_near.wait_recv()
        g_pass.wait_recv()
        gates = gbuf[layer]
        row_lane = lax.broadcasted_iota(jnp.int32, (rows, LANES), 1)
        for k in range(local):
            one = jnp.sum(jnp.where(row_lane == e * local + k, gates, 0.0), axis=1, keepdims=True)
            gsel[k] = jnp.broadcast_to(one, (rows, LANES))

        def near_l(j):
            return remote(stage.at[j, pl.ds(toks, toks)], part_l.at[layer, j], ps.at[j], pr.at[layer, j], "ep", partner)

        def near_m(j):
            return remote(stage.at[j, pl.ds(3 * toks, toks)], part_m.at[layer, j], ms.at[j], mr.at[layer, j], "ep", partner)

        def far_copy(j):
            return remote(merged.at[j], far.at[layer, j], fs.at[j], fr.at[layer, j], "ep", cross)

        def merge(j):
            near_m(j).wait_recv()
            merged[j] = stage[j, pl.ds(2 * toks, toks), :] + part_m[layer, j]
            far_copy(j).start()

        def combine(c):
            near_l(c).wait_recv()
            far_copy(c).wait_recv()
            total = (stage[c, pl.ds(0, toks), :] + part_l[layer, c]) + far[layer, c]
            x = (acc_a[:, columns(c)].astype(jnp.float32) + total).astype(jnp.bfloat16)
            acc_a[:, columns(c)] = x

            @pl.when(layer == layers - 1)
            def _():
                xg[p, :, columns(c)] = x
                store(p, c).start()

                for way in WAYS:
                    @pl.when((p + way >= 0) & (p + way < pools))
                    def _(way=way):
                        spread_out(p, c, way).start()

        def down(j, slot, low):
            terms = [None] * (DOWN_COLS // LANES)
            for k in range(local):
                y = jnp.dot(inner[k, low:low + 2 * toks, :], dbuf[slot, k], preferred_element_type=jnp.float32)
                y = y.astype(jnp.bfloat16).astype(jnp.float32)
                gate = gsel[k, low:low + 2 * toks, :]
                for n in range(len(terms)):
                    term = jnp.where(gate > 0.0, gate * y[:, n * LANES:(n + 1) * LANES], 0.0)
                    terms[n] = term if k == 0 else terms[n] + term
            for n in range(len(terms)):
                stage[j, low:low + 2 * toks, n * LANES:(n + 1) * LANES] = terms[n]

        def down_far(j):
            for c in d_copies(layer * d_chunks + j):
                c.wait()
            down(j, j % DOWN_SLOTS, 2 * toks)
            near_m(j).start()

        def down_body(j, carry):
            d = layer * d_chunks + j

            @pl.when(j + 1 < d_chunks)
            def _():
                down_far(j + 1)

            merge(j)
            down(j, j % DOWN_SLOTS, 0)
            near_l(j).start()

            @pl.when(j + DOWN_SLOTS < d_chunks)
            def _():
                for c in d_copies(d + DOWN_SLOTS):
                    c.start()

            @pl.when((j == ATTENTION_AT) & (layer + 1 < layers))
            def _():
                start_attention(layer + 1)

            @pl.when(j >= LAG)
            def _():
                combine(j - LAG)

            return carry

        down_far(0)
        lax.fori_loop(0, d_chunks, down_body, 0)

        @pl.when(layer + 1 < layers)
        def _():
            start_gate_up(layer + 1)
            start_down(layer + 1)


        def last_ones(c, carry):
            combine(c)

            @pl.when(layer == layers - 1)
            def _():
                relay(c - RELAY_LAG)

            return carry

        lax.fori_loop(d_chunks - LAG, d_chunks, last_ones, 0)

        for c in u_near + u_far + u_pass + [g_near, g_far, g_pass]:
            c.wait_send()

        def sent(j, carry):
            near_l(j).wait_send()
            near_m(j).wait_send()
            far_copy(j).wait_send()
            return carry

        lax.fori_loop(0, d_chunks, sent, 0)
        return carry

    def spread_out(origin, c, way, kind=None):
        at = xg.at[origin, :, columns(c)]
        return remote(at, at, zs.at[WAYS.index(way) if kind is None else kind, c], zr.at[origin, c], "pool", p + way)

    def store(origin, c):
        here = pl.ds(origin * toks, toks)
        return pltpu.make_async_copy(xg.at[origin, :, columns(c)], out.at[here, columns(c)], osem.at[0])

    def relay(c):
        @pl.when(p == 1)
        def _():
            received(3, c, 2)
            spread_out(3, c, -1, len(WAYS)).start()
            store(3, c).start()

        @pl.when(p == 2)
        def _():
            received(0, c, -2)
            spread_out(0, c, 1, len(WAYS)).start()
            store(0, c).start()

    def received(origin, c, way):
        spread_out(origin, c, way).wait_recv()

    lax.fori_loop(0, layers, layer_body, 0)

    def rest(c, carry):
        @pl.when(c + RELAY_LAG >= d_chunks)
        def _():
            relay(c)

        for step in range(1, pools):
            for origin, way in ((p - step, -1), (p + step, 1)):
                via_relay = ((p == 1) & (origin == 3)) | ((p == 2) & (origin == 0))

                @pl.when((origin >= 0) & (origin < pools) & jnp.logical_not(via_relay))
                def _(origin=origin, way=way):
                    received(origin, c, way)
                    store(origin, c).start()

        return carry

    lax.fori_loop(0, d_chunks, rest, 0)

    def finish(c, carry):
        for way in WAYS:
            @pl.when((p + way >= 0) & (p + way < pools))
            def _(way=way):
                spread_out(p, c, way).wait_send()

        @pl.when(p == 1)
        def _():
            spread_out(3, c, -1, len(WAYS)).wait_send()

        @pl.when(p == 2)
        def _():
            spread_out(0, c, 1, len(WAYS)).wait_send()

        return carry

    lax.fori_loop(0, d_chunks, finish, 0)
    pltpu.make_async_copy(out, out, osem.at[0]).wait()


def solution(mesh):
    pools = mesh.shape["pool"]

    def body(hidden, k_cache, v_cache, lengths, expert_ids, w_query, w_key, w_value, w_out, w_router, w_gate, w_up, w_down):
        layers, shard, seq, kv_heads, head = k_cache.shape
        model = hidden.shape[1]
        toks = shard // pools
        local, ff = w_gate.shape[1], w_gate.shape[3]
        heads = w_query.shape[2] // head
        dims = (layers, toks, model, ff, heads, local)
        cos_t, sin_t = rotary_tables(seq + 8)
        f32, bf16 = jnp.float32, jnp.bfloat16
        d_chunks = model // DOWN_COLS
        dma, vmem = pltpu.SemaphoreType.DMA, pltpu.VMEM
        scratch = [
            vmem((heads * head, model), bf16),
            vmem((toks, seq * kv_heads, head), bf16), vmem((toks, seq * kv_heads, head), bf16),
            vmem((GU_SLOTS, 2, model, GU_COLS), bf16), vmem((DOWN_SLOTS, local, ff, DOWN_COLS), bf16),
            vmem((layers, 4 * toks, model), bf16), vmem((local, 4 * toks, ff), bf16),
            vmem((d_chunks, 4 * toks, DOWN_COLS), f32),
            vmem((layers, d_chunks, toks, DOWN_COLS), f32), vmem((layers, d_chunks, toks, DOWN_COLS), f32),
            vmem((d_chunks, toks, DOWN_COLS), f32), vmem((layers, d_chunks, toks, DOWN_COLS), f32),
            vmem((pools, toks, model), bf16), vmem((toks, model), bf16),
            vmem((16 * toks, head), f32), vmem((16 * toks, head), f32), vmem((16 * toks, head), f32), vmem((16 * toks, head), f32),
            vmem((GROUP * 16, seq * kv_heads), f32), vmem((GROUP * 16, seq * kv_heads), f32),
            vmem((toks, heads * head), bf16), vmem((layers, 4 * toks, LANES), f32), vmem((local, 4 * toks, LANES), f32),
            vmem((layers, w_router.shape[2], model), f32),
            vmem(cos_t.shape, f32), vmem(sin_t.shape, f32), vmem((toks, head), f32), vmem((toks, head), f32),
            vmem((layers, 2, toks, LANES), jnp.int32),
            dma((3 + heads * head // CHUNK,)), dma((KV_BLOCKS, 2)), dma((GU_SLOTS, 2)), dma((DOWN_SLOTS, local)), dma((4,)),
            dma((3, 2)), dma((layers, 3, 2)), dma((3,)), dma((layers, 3)),
            dma((d_chunks,)), dma((layers, d_chunks)), dma((d_chunks,)), dma((layers, d_chunks)),
            dma((d_chunks,)), dma((layers, d_chunks)), dma((len(WAYS) + 1, d_chunks)), dma((pools, d_chunks)), dma((1,)),
        ]
        smem = pl.BlockSpec(memory_space=pltpu.SMEM)
        anyw = pl.BlockSpec(memory_space=pl.ANY)
        return pl.pallas_call(
            functools.partial(kernel, dims),
            out_shape=jax.ShapeDtypeStruct((shard, model), bf16),
            in_specs=[smem, smem] + [anyw] * 13,
            out_specs=anyw,
            scratch_shapes=scratch,
            compiler_params=pltpu.CompilerParams(collective_id=0, has_side_effects=True, vmem_limit_bytes=67043328),
            name="decode",
        )(lengths, jnp.swapaxes(expert_ids, 1, 2), hidden,
          k_cache.reshape(layers, shard, seq * kv_heads, head), v_cache.reshape(layers, shard, seq * kv_heads, head),
          w_query, w_key, w_value, w_out, jnp.swapaxes(w_router, 1, 2), jnp.asarray(cos_t), jnp.asarray(sin_t),
          w_gate, w_up, w_down)

    rows_spec = ("dp", "ep")
    in_specs = (P(rows_spec, None), P(None, rows_spec), P(None, rows_spec), P(rows_spec), P(None, rows_spec, None), P(), P(), P(), P(), P(), P(None, "ep"), P(None, "ep"), P(None, "ep"))
    return jax.shard_map(body, mesh=mesh, in_specs=in_specs, out_specs=P(rows_spec, None), check_vma=False)
```

```python
import functools
import math

import jax
import jax.numpy as jnp
import numpy as np
from jax import lax
from jax.experimental import pallas as pl
from jax.experimental.pallas import tpu as pltpu
from jax.sharding import PartitionSpec as P

EPSILON = 1e-6
ROPE_BASE = 10000.0
MESH = pl.DeviceIdType.MESH
HEAD = 128
KV = 2
LANES = 128
CHUNK = 512
GU_COLS = 1024
GU_SLOTS = 4
PIECE = 256
DOWN_SLOTS = 3
DOWN_COLS = 256
KV_BLOCKS = 4
GROUP = 8
LAG = 4
ATTENTION_AT = 3
WAYS = (-2, 2, -1, 1)
RELAY_LAG = 2


def rotary_tables(size):
    half = HEAD // 2
    freqs = np.float32(ROPE_BASE) ** (np.float32(-2.0) * np.arange(half, dtype=np.float32) / np.float32(HEAD))
    angle = np.arange(size, dtype=np.float32)[:, None] * freqs[None, :].astype(np.float32)
    cosine = np.cos(angle).astype(np.float32)
    sine = np.sin(angle).astype(np.float32)
    return np.concatenate([cosine, cosine], 1), np.concatenate([-sine, sine], 1)


def normed(values):
    return values * lax.rsqrt(jnp.mean(values * values, axis=-1, keepdims=True) + EPSILON)


def kernel(dims, lens_h, ids_h, hid, kc, vc, wq, wk, wv, wo, wr, cos_t, sin_t, wg, wu, wd, out,
           wo_b, kbuf, vbuf, gu, dbuf, ubuf, inner, stage, part_l, part_m, merged, far, xg, acc_a,
           q2d, k2d, v2d, o2d, s_even, s_odd, att, gbuf, gsel, wr_b, lens, ids, cosb, sinb, cosr, sinr, id_b,
           wsem, kvsem, gusem, dsem, isem, us, ur, gs, gr, ps, pr, ms, mr, fs, fr, zs, zr, osem):
    layers, toks, model, ff, heads, local = dims
    e = lax.axis_index("ep")
    p = lax.axis_index("pool")
    pools = 4
    partner = e + 1 - 2 * (e % 2)
    cross = (e + 2) % 4
    start = p * toks
    ff_chunks = ff // GU_COLS
    gu_total = local * ff_chunks
    d_chunks = model // DOWN_COLS
    rows = 4 * toks
    half = toks // 2
    group = heads // KV
    seq2 = kbuf.shape[1]
    per_block = toks // KV_BLOCKS

    def remote(src, dst, ssem, rsem, axis, index):
        return pltpu.make_async_remote_copy(src_ref=src, dst_ref=dst, send_sem=ssem, recv_sem=rsem,
                                            device_id={axis: index}, device_id_type=MESH)

    def columns(j):
        return pl.ds(pl.multiple_of(j * DOWN_COLS, DOWN_COLS), DOWN_COLS)

    def gu_copies(g):
        layer, i, slot = g // gu_total, g % gu_total, (g % gu_total) % GU_SLOTS
        expert, c = i // ff_chunks, i % ff_chunks
        cols = pl.ds(pl.multiple_of(c * GU_COLS, GU_COLS), GU_COLS)
        return [pltpu.make_async_copy(w.at[layer, expert, :, cols], gu.at[slot, k], gusem.at[slot, k])
                for k, w in enumerate((wg, wu))]

    def d_copies(d):
        layer, j, slot = d // d_chunks, d % d_chunks, (d % d_chunks) % DOWN_SLOTS
        return [pltpu.make_async_copy(wd.at[layer, k, :, columns(j)], dbuf.at[slot, k], dsem.at[slot, k]) for k in range(local)]

    kvw = KV * HEAD
    q_cols = heads * HEAD

    def proj(column, count):
        return gu.at[GU_SLOTS - 1, column // GU_COLS, :, pl.ds(column % GU_COLS, count)]

    def weight_copies(layer):
        pieces = range(q_cols // CHUNK)
        return [pltpu.make_async_copy(wk.at[layer], proj(q_cols, kvw), wsem.at[0]),
                pltpu.make_async_copy(wv.at[layer], proj(q_cols + kvw, kvw), wsem.at[1]),
                pltpu.make_async_copy(wo.at[layer], wo_b, wsem.at[2]),
                *(pltpu.make_async_copy(wq.at[layer, :, pl.ds(n * CHUNK, CHUNK)], proj(n * CHUNK, CHUNK), wsem.at[3 + n]) for n in pieces)]

    def kv_copies(layer, b):
        here = pl.ds(start + b * per_block, per_block)
        there = pl.ds(b * per_block, per_block)
        return [pltpu.make_async_copy(kc.at[layer, here], kbuf.at[there], kvsem.at[b, 0]),
                pltpu.make_async_copy(vc.at[layer, here], vbuf.at[there], kvsem.at[b, 1])]

    def start_projections(layer):
        copies = weight_copies(layer)
        for c in copies[3:] + copies[:2]:
            c.start()

    def start_caches(layer):
        for b in range(KV_BLOCKS):
            for c in kv_copies(layer, b):
                c.start()
        weight_copies(layer)[2].start()

    def start_attention(layer):
        start_projections(layer)
        start_caches(layer)

    def start_gate_up(layer):
        for i in range(GU_SLOTS - 1):
            for c in gu_copies(layer * gu_total + i):
                c.start()

    def start_down(layer):
        for j in range(DOWN_SLOTS):
            for c in d_copies(layer * d_chunks + j):
                c.start()

    first = [pltpu.make_async_copy(hid.at[pl.ds(start, toks)], acc_a, isem.at[0]),
             pltpu.make_async_copy(wr, wr_b, isem.at[1]),
             pltpu.make_async_copy(cos_t, cosb, isem.at[2]),
             pltpu.make_async_copy(sin_t, sinb, isem.at[3]),
             pltpu.make_async_copy(lens_h, lens, isem.at[4]),
             pltpu.make_async_copy(ids_h, ids, isem.at[5])]
    for c in first:
        c.start()
    start_attention(0)
    start_gate_up(0)
    start_down(0)

    barrier = pltpu.get_barrier_semaphore()
    pl.semaphore_signal(barrier, inc=1, device_id={"ep": partner}, device_id_type=MESH)
    pl.semaphore_signal(barrier, inc=1, device_id={"ep": cross}, device_id_type=MESH)

    inside = (p > 0) & (p < pools - 1)
    for way in (-2, -1, 1, 2):
        @pl.when((p + way >= 0) & (p + way < pools))
        def _(way=way):
            pl.semaphore_signal(barrier, inc=1, device_id={"pool": p + way}, device_id_type=MESH)

    with jax.named_scope("firstwait"):
        for c in first:
            c.wait()

    zeros = jnp.zeros(((16 - heads) * toks, HEAD), jnp.float32)
    for ref in (q2d, k2d, v2d):
        ref[pl.ds(heads * toks, (16 - heads) * toks), :] = zeros

    def spread(t, carry):
        where = pl.ds(t, 1)
        n = lens[start + t]
        cosr[where, :] = cosb[pl.ds(n, 1), :]
        sinr[where, :] = sinb[pl.ds(n, 1), :]
        for layer in range(layers):
            for k in range(2):
                id_b[layer, k, where, :] = jnp.full((1, LANES), ids[layer, k, start + t], jnp.int32)
        return carry

    with jax.named_scope("spread"):
        lax.fori_loop(0, toks, spread, 0)

    lane = lax.broadcasted_iota(jnp.int32, (16, seq2), 1)
    head_kv = jnp.where(lax.broadcasted_iota(jnp.int32, (16, seq2), 0) >= group, 1, 0)
    parity = (lane % KV) == head_kv
    scale = HEAD ** -0.5

    def layer_body(layer, carry):
        with jax.named_scope("qkv"):
            hidden = acc_a[...].astype(jnp.float32)
            h = normed(hidden).astype(jnp.bfloat16)
            copies = weight_copies(layer)
            for c in copies[3:] + copies[:2]:
                c.wait()
            cosine, sine = cosr[...], sinr[...]

            def rope(v):
                return (v * cosine + pltpu.roll(v, HEAD // 2, 1) * sine).astype(jnp.bfloat16).astype(jnp.float32)

            for n in range(heads * HEAD // CHUNK):
                qn = jnp.dot(h, proj(n * CHUNK, CHUNK)[...], preferred_element_type=jnp.float32)
                for k in range(CHUNK // HEAD):
                    head = n * (CHUNK // HEAD) + k
                    q2d[pl.ds(head * toks, toks), :] = rope(qn[:, k * HEAD:(k + 1) * HEAD])
            kv = jnp.dot(h, proj(q_cols, 2 * kvw)[...], preferred_element_type=jnp.float32)
            for j in range(KV):
                kj = rope(kv[:, j * HEAD:(j + 1) * HEAD])
                vj = kv[:, kvw + j * HEAD:kvw + (j + 1) * HEAD].astype(jnp.bfloat16).astype(jnp.float32)
                for k in range(group):
                    at = pl.ds((j * group + k) * toks, toks)
                    k2d[at, :] = kj
                    v2d[at, :] = vj

        for c in gu_copies(layer * gu_total + GU_SLOTS - 1):
            c.start()

        def score(first_token, ref):
            for k in range(GROUP):
                q = q2d[pl.ds(first_token + k, 16, stride=toks), :].astype(jnp.bfloat16)
                ref[k * 16:(k + 1) * 16, :] = lax.dot_general(q, kbuf[first_token + k], (((1,), (1,)), ((), ())),
                                                              preferred_element_type=jnp.float32)

        def mix(first_token, ref):
            weights, news, totals = [], [], []
            for k in range(GROUP):
                at = pl.ds(first_token + k, 16, stride=toks)
                n2 = lens[start + first_token + k] * KV
                s = jnp.where(parity & (lane < n2), ref[k * 16:(k + 1) * 16, :] * scale, -jnp.inf)
                s_new = jnp.sum(q2d[at, :] * k2d[at, :], axis=1, keepdims=True) * scale
                peak = jnp.maximum(jnp.max(s, axis=1, keepdims=True), s_new)
                w = jnp.exp(s - peak)
                w_new = jnp.exp(s_new - peak)
                totals.append(jnp.sum(w, axis=1, keepdims=True) + w_new)
                weights.append(w.astype(jnp.bfloat16))
                news.append(w_new.astype(jnp.bfloat16).astype(jnp.float32))
            sums = [jnp.dot(weights[k], vbuf[first_token + k], preferred_element_type=jnp.float32) for k in range(GROUP)]
            for k in range(GROUP):
                at = pl.ds(first_token + k, 16, stride=toks)
                o2d[at, :] = (sums[k] + news[k] * v2d[at, :]) / totals[k]

        with jax.named_scope("attn"):
            kv_copies(layer, 0)[0].wait()
            score(0, s_even)

            def attend(i, carry):
                kv_copies(layer, i)[1].wait()

                @pl.when(i + 1 < KV_BLOCKS)
                def _():
                    kv_copies(layer, i + 1)[0].wait()

                t = i * per_block
                score(t + GROUP, s_odd)
                mix(t, s_even)
                score((t + 2 * GROUP) % toks, s_even)
                mix(t + GROUP, s_odd)
                return carry

            lax.fori_loop(0, KV_BLOCKS, attend, 0)

        with jax.named_scope("wo"):
            for head in range(heads):
                att[:, head * HEAD:(head + 1) * HEAD] = o2d[pl.ds(head * toks, toks), :].astype(jnp.bfloat16)
            copies[2].wait()
            for n in range(model // CHUNK):
                cols = slice(n * CHUNK, (n + 1) * CHUNK)
                a = acc_a[:, cols].astype(jnp.float32) + jnp.dot(att[...], wo_b[:, cols], preferred_element_type=jnp.float32)
                acc_a[:, cols] = a.astype(jnp.bfloat16)

        u = normed(acc_a[...].astype(jnp.float32)).astype(jnp.bfloat16)
        ubuf[layer, pl.ds(0, toks), :] = u

        def block(ref, b):
            return ref.at[layer, pl.ds(b * toks, toks)]

        def piece(b, h):
            return ubuf.at[layer, pl.ds(b * toks + h * half, half)]

        u_near = [remote(piece(0, h), piece(1, h), us.at[0, h], ur.at[layer, 0, h], "ep", partner) for h in range(2)]
        u_far = [remote(piece(0, h), piece(2, h), us.at[1, h], ur.at[layer, 1, h], "ep", cross) for h in range(2)]
        u_pass = [remote(piece(2, h), piece(3, h), us.at[2, h], ur.at[layer, 2, h], "ep", partner) for h in range(2)]
        g_near = remote(block(gbuf, 0), block(gbuf, 1), gs.at[0], gr.at[layer, 0], "ep", partner)
        g_far = remote(block(gbuf, 0), block(gbuf, 2), gs.at[1], gr.at[layer, 1], "ep", cross)
        g_pass = remote(block(gbuf, 2), block(gbuf, 3), gs.at[2], gr.at[layer, 2], "ep", partner)
        @pl.when((layer == 0) & inside)
        def _():
            pl.semaphore_wait(barrier, 5)

        @pl.when((layer == 0) & jnp.logical_not(inside))
        def _():
            pl.semaphore_wait(barrier, 4)

        for c in u_far + u_near:
            c.start()

        wl = wr_b[layer]
        hi = wl.astype(jnp.bfloat16).astype(jnp.float32)
        rest = wl - hi
        mid = rest.astype(jnp.bfloat16).astype(jnp.float32)
        low = rest - mid
        wide = jnp.concatenate([hi, mid, low, jnp.zeros((LANES - 3 * wl.shape[0], model), jnp.float32)], axis=0).astype(jnp.bfloat16)
        parts = lax.dot_general(u, wide, (((1,), (1,)), ((), ())), preferred_element_type=jnp.float32)
        logits = parts + pltpu.roll(parts, LANES - 8, 1) + pltpu.roll(parts, LANES - 16, 1)
        expert_lane = lax.broadcasted_iota(jnp.int32, (toks, LANES), 1)
        chosen = (id_b[layer, 0] == expert_lane) | (id_b[layer, 1] == expert_lane)
        logits = jnp.where(chosen, logits, -jnp.inf)
        ew = jnp.exp(logits - jnp.max(logits, axis=1, keepdims=True))
        gbuf[layer, pl.ds(0, toks), :] = ew / jnp.sum(ew, axis=1, keepdims=True)
        g_far.start()
        g_near.start()

        def gate_up(low, count, wait, release):
            def step(i, carry):
                g = layer * gu_total + i
                slot = i % GU_SLOTS
                if wait:
                    for c in gu_copies(g):
                        c.wait()
                for n in range(0, GU_COLS, PIECE):
                    tokens = ubuf[layer, low:low + count, :]
                    one = jnp.dot(tokens, gu[slot, 0, :, n:n + PIECE], preferred_element_type=jnp.float32)
                    three = jnp.dot(tokens, gu[slot, 1, :, n:n + PIECE], preferred_element_type=jnp.float32)
                    cols = pl.ds(pl.multiple_of((i % ff_chunks) * GU_COLS + n, PIECE), PIECE)
                    inner[i // ff_chunks, low:low + count, cols] = (jax.nn.silu(one) * three).astype(jnp.bfloat16)
                if release:
                    @pl.when(i + GU_SLOTS < gu_total)
                    def _():
                        for c in gu_copies(g + GU_SLOTS):
                            c.start()

                return carry

            return step

        with jax.named_scope("nearwait"):
            for c in u_near:
                c.wait_recv()

        with jax.named_scope("l1"):
            lax.fori_loop(0, 2, gate_up(0, 2 * toks, True, False), 0)

        with jax.named_scope("farwait0"):
            u_far[0].wait_recv()

        u_pass[0].start()
        with jax.named_scope("l2"):
            lax.fori_loop(2, GU_SLOTS, gate_up(0, 2 * toks, True, False), 0)

        with jax.named_scope("farwait1"):
            u_far[1].wait_recv()

        u_pass[1].start()
        g_far.wait_recv()
        g_pass.start()
        with jax.named_scope("passwait"):
            for c in u_pass:
                c.wait_recv()

        with jax.named_scope("r"):
            lax.fori_loop(0, GU_SLOTS, gate_up(2 * toks, 2 * toks, False, True), 0)

        with jax.named_scope("main"):
            lax.fori_loop(GU_SLOTS, gu_total, gate_up(0, 4 * toks, True, True), 0)

        g_near.wait_recv()
        g_pass.wait_recv()
        gates = gbuf[layer]
        row_lane = lax.broadcasted_iota(jnp.int32, (rows, LANES), 1)
        for k in range(local):
            one = jnp.sum(jnp.where(row_lane == e * local + k, gates, 0.0), axis=1, keepdims=True)
            gsel[k] = jnp.broadcast_to(one, (rows, LANES))

        def near_l(j):
            return remote(stage.at[j, pl.ds(toks, toks)], part_l.at[layer, j], ps.at[j], pr.at[layer, j], "ep", partner)

        def near_m(j):
            return remote(stage.at[j, pl.ds(3 * toks, toks)], part_m.at[layer, j], ms.at[j], mr.at[layer, j], "ep", partner)

        def far_copy(j):
            return remote(merged.at[j], far.at[layer, j], fs.at[j], fr.at[layer, j], "ep", cross)

        def merge(j):
            near_m(j).wait_recv()
            merged[j] = stage[j, pl.ds(2 * toks, toks), :] + part_m[layer, j]
            far_copy(j).start()

        def combine(c):
            near_l(c).wait_recv()
            far_copy(c).wait_recv()
            total = (stage[c, pl.ds(0, toks), :] + part_l[layer, c]) + far[layer, c]
            x = (acc_a[:, columns(c)].astype(jnp.float32) + total).astype(jnp.bfloat16)
            acc_a[:, columns(c)] = x

            @pl.when(layer == layers - 1)
            def _():
                xg[p, :, columns(c)] = x
                store(p, c).start()

                for way in WAYS:
                    @pl.when((p + way >= 0) & (p + way < pools))
                    def _(way=way):
                        spread_out(p, c, way).start()

        def down(j, slot, low):
            terms = [None] * (DOWN_COLS // LANES)
            for k in range(local):
                y = jnp.dot(inner[k, low:low + 2 * toks, :], dbuf[slot, k], preferred_element_type=jnp.float32)
                y = y.astype(jnp.bfloat16).astype(jnp.float32)
                gate = gsel[k, low:low + 2 * toks, :]
                for n in range(len(terms)):
                    term = jnp.where(gate > 0.0, gate * y[:, n * LANES:(n + 1) * LANES], 0.0)
                    terms[n] = term if k == 0 else terms[n] + term
            for n in range(len(terms)):
                stage[j, low:low + 2 * toks, n * LANES:(n + 1) * LANES] = terms[n]

        def down_far(j):
            for c in d_copies(layer * d_chunks + j):
                c.wait()
            down(j, j % DOWN_SLOTS, 2 * toks)
            near_m(j).start()

        def down_body(j, carry):
            d = layer * d_chunks + j

            @pl.when(j + 1 < d_chunks)
            def _():
                down_far(j + 1)

            merge(j)
            down(j, j % DOWN_SLOTS, 0)
            near_l(j).start()

            @pl.when(j + DOWN_SLOTS < d_chunks)
            def _():
                for c in d_copies(d + DOWN_SLOTS):
                    c.start()

            @pl.when((j == ATTENTION_AT) & (layer + 1 < layers))
            def _():
                start_attention(layer + 1)

            @pl.when(j >= LAG)
            def _():
                combine(j - LAG)

            return carry

        with jax.named_scope("down"):
            down_far(0)
            lax.fori_loop(0, d_chunks, down_body, 0)

        @pl.when(layer + 1 < layers)
        def _():
            start_gate_up(layer + 1)
            start_down(layer + 1)


        def last_ones(c, carry):
            combine(c)

            @pl.when(layer == layers - 1)
            def _():
                relay(c - RELAY_LAG)

            return carry

        with jax.named_scope("tail"):
            lax.fori_loop(d_chunks - LAG, d_chunks, last_ones, 0)

        for c in u_near + u_far + u_pass + [g_near, g_far, g_pass]:
            c.wait_send()

        def sent(j, carry):
            near_l(j).wait_send()
            near_m(j).wait_send()
            far_copy(j).wait_send()
            return carry

        lax.fori_loop(0, d_chunks, sent, 0)
        return carry

    def spread_out(origin, c, way, kind=None):
        at = xg.at[origin, :, columns(c)]
        return remote(at, at, zs.at[WAYS.index(way) if kind is None else kind, c], zr.at[origin, c], "pool", p + way)

    def store(origin, c):
        here = pl.ds(origin * toks, toks)
        return pltpu.make_async_copy(xg.at[origin, :, columns(c)], out.at[here, columns(c)], osem.at[0])

    def relay(c):
        @pl.when(p == 1)
        def _():
            received(3, c, 2)
            spread_out(3, c, -1, len(WAYS)).start()
            store(3, c).start()

        @pl.when(p == 2)
        def _():
            received(0, c, -2)
            spread_out(0, c, 1, len(WAYS)).start()
            store(0, c).start()

    def received(origin, c, way):
        spread_out(origin, c, way).wait_recv()

    lax.fori_loop(0, layers, layer_body, 0)

    def rest(c, carry):
        @pl.when(c + RELAY_LAG >= d_chunks)
        def _():
            relay(c)

        for step in range(1, pools):
            for origin, way in ((p - step, -1), (p + step, 1)):
                via_relay = ((p == 1) & (origin == 3)) | ((p == 2) & (origin == 0))

                @pl.when((origin >= 0) & (origin < pools) & jnp.logical_not(via_relay))
                def _(origin=origin, way=way):
                    received(origin, c, way)
                    store(origin, c).start()

        return carry

    with jax.named_scope("rest"):
        lax.fori_loop(0, d_chunks, rest, 0)

    def finish(c, carry):
        for way in WAYS:
            @pl.when((p + way >= 0) & (p + way < pools))
            def _(way=way):
                spread_out(p, c, way).wait_send()

        @pl.when(p == 1)
        def _():
            spread_out(3, c, -1, len(WAYS)).wait_send()

        @pl.when(p == 2)
        def _():
            spread_out(0, c, 1, len(WAYS)).wait_send()

        return carry

    with jax.named_scope("finish"):
        lax.fori_loop(0, d_chunks, finish, 0)
        pltpu.make_async_copy(out, out, osem.at[0]).wait()


def solution(mesh):
    pools = mesh.shape["pool"]

    def body(hidden, k_cache, v_cache, lengths, expert_ids, w_query, w_key, w_value, w_out, w_router, w_gate, w_up, w_down):
        layers, shard, seq, kv_heads, head = k_cache.shape
        model = hidden.shape[1]
        toks = shard // pools
        local, ff = w_gate.shape[1], w_gate.shape[3]
        heads = w_query.shape[2] // head
        dims = (layers, toks, model, ff, heads, local)
        cos_t, sin_t = rotary_tables(seq + 8)
        f32, bf16 = jnp.float32, jnp.bfloat16
        d_chunks = model // DOWN_COLS
        dma, vmem = pltpu.SemaphoreType.DMA, pltpu.VMEM
        scratch = [
            vmem((heads * head, model), bf16),
            vmem((toks, seq * kv_heads, head), bf16), vmem((toks, seq * kv_heads, head), bf16),
            vmem((GU_SLOTS, 2, model, GU_COLS), bf16), vmem((DOWN_SLOTS, local, ff, DOWN_COLS), bf16),
            vmem((layers, 4 * toks, model), bf16), vmem((local, 4 * toks, ff), bf16),
            vmem((d_chunks, 4 * toks, DOWN_COLS), f32),
            vmem((layers, d_chunks, toks, DOWN_COLS), f32), vmem((layers, d_chunks, toks, DOWN_COLS), f32),
            vmem((d_chunks, toks, DOWN_COLS), f32), vmem((layers, d_chunks, toks, DOWN_COLS), f32),
            vmem((pools, toks, model), bf16), vmem((toks, model), bf16),
            vmem((16 * toks, head), f32), vmem((16 * toks, head), f32), vmem((16 * toks, head), f32), vmem((16 * toks, head), f32),
            vmem((GROUP * 16, seq * kv_heads), f32), vmem((GROUP * 16, seq * kv_heads), f32),
            vmem((toks, heads * head), bf16), vmem((layers, 4 * toks, LANES), f32), vmem((local, 4 * toks, LANES), f32),
            vmem((layers, w_router.shape[2], model), f32),
            pltpu.SMEM((shard,), jnp.int32), pltpu.SMEM((layers, 2, shard), jnp.int32),
            vmem(cos_t.shape, f32), vmem(sin_t.shape, f32), vmem((toks, head), f32), vmem((toks, head), f32),
            vmem((layers, 2, toks, LANES), jnp.int32),
            dma((3 + heads * head // CHUNK,)), dma((KV_BLOCKS, 2)), dma((GU_SLOTS, 2)), dma((DOWN_SLOTS, local)), dma((6,)),
            dma((3, 2)), dma((layers, 3, 2)), dma((3,)), dma((layers, 3)),
            dma((d_chunks,)), dma((layers, d_chunks)), dma((d_chunks,)), dma((layers, d_chunks)),
            dma((d_chunks,)), dma((layers, d_chunks)), dma((len(WAYS) + 1, d_chunks)), dma((pools, d_chunks)), dma((1,)),
        ]
        anyw = pl.BlockSpec(memory_space=pl.ANY)
        return pl.pallas_call(
            functools.partial(kernel, dims),
            out_shape=jax.ShapeDtypeStruct((shard, model), bf16),
            in_specs=[anyw] * 15,
            out_specs=anyw,
            scratch_shapes=scratch,
            compiler_params=pltpu.CompilerParams(collective_id=0, has_side_effects=True, vmem_limit_bytes=67043328),
            name="decode",
        )(lengths, jnp.swapaxes(expert_ids, 1, 2), hidden,
          k_cache.reshape(layers, shard, seq * kv_heads, head), v_cache.reshape(layers, shard, seq * kv_heads, head),
          w_query, w_key, w_value, w_out, jnp.swapaxes(w_router, 1, 2), jnp.asarray(cos_t), jnp.asarray(sin_t),
          w_gate, w_up, w_down)

    rows_spec = ("dp", "ep")
    in_specs = (P(rows_spec, None), P(None, rows_spec), P(None, rows_spec), P(rows_spec), P(None, rows_spec, None), P(), P(), P(), P(), P(), P(None, "ep"), P(None, "ep"), P(None, "ep"))
    return jax.shard_map(body, mesh=mesh, in_specs=in_specs, out_specs=P(rows_spec, None), check_vma=False)
```

```python
import functools
import math

import jax
import jax.numpy as jnp
import numpy as np
from jax import lax
from jax.experimental import pallas as pl
from jax.experimental.pallas import tpu as pltpu
from jax.sharding import PartitionSpec as P

EPSILON = 1e-6
ROPE_BASE = 10000.0
MESH = pl.DeviceIdType.MESH
HEAD = 128
KV = 2
LANES = 128
CHUNK = 512
GU_COLS = 1024
GU_SLOTS = 4
PIECE = 256
DOWN_SLOTS = 3
DOWN_COLS = 256
KV_BLOCKS = 4
GROUP = 8
LAG = 3
ATTENTION_AT = 3
WAYS = (-2, 2, -1, 1)
RELAY_LAG = 3


def rotary_tables(size):
    half = HEAD // 2
    freqs = np.float32(ROPE_BASE) ** (np.float32(-2.0) * np.arange(half, dtype=np.float32) / np.float32(HEAD))
    angle = np.arange(size, dtype=np.float32)[:, None] * freqs[None, :].astype(np.float32)
    cosine = np.cos(angle).astype(np.float32)
    sine = np.sin(angle).astype(np.float32)
    return np.concatenate([cosine, cosine], 1), np.concatenate([-sine, sine], 1)


def normed(values):
    return values * lax.rsqrt(jnp.mean(values * values, axis=-1, keepdims=True) + EPSILON)


def kernel(dims, lens_h, ids_h, hid, kc, vc, wq, wk, wv, wo, wr, cos_t, sin_t, wg, wu, wd, out,
           wo_b, kbuf, vbuf, gu, dbuf, ubuf, inner, stage, part_l, part_m, merged, far, xg, acc_a,
           q2d, k2d, v2d, o2d, s_even, s_odd, att, gbuf, gsel, wr_b, lens, ids, cosb, sinb, cosr, sinr, id_b,
           wsem, kvsem, gusem, dsem, isem, us, ur, gs, gr, ps, pr, ms, mr, fs, fr, zs, zr, osem):
    layers, toks, model, ff, heads, local = dims
    e = lax.axis_index("ep")
    p = lax.axis_index("pool")
    pools = 4
    partner = e + 1 - 2 * (e % 2)
    cross = (e + 2) % 4
    start = p * toks
    ff_chunks = ff // GU_COLS
    gu_total = local * ff_chunks
    d_chunks = model // DOWN_COLS
    rows = 4 * toks
    half = toks // 2
    group = heads // KV
    seq2 = kbuf.shape[1]
    per_block = toks // KV_BLOCKS

    def remote(src, dst, ssem, rsem, axis, index):
        return pltpu.make_async_remote_copy(src_ref=src, dst_ref=dst, send_sem=ssem, recv_sem=rsem,
                                            device_id={axis: index}, device_id_type=MESH)

    def columns(j):
        return pl.ds(pl.multiple_of(j * DOWN_COLS, DOWN_COLS), DOWN_COLS)

    def gu_copies(g):
        layer, i, slot = g // gu_total, g % gu_total, (g % gu_total) % GU_SLOTS
        expert, c = i // ff_chunks, i % ff_chunks
        cols = pl.ds(pl.multiple_of(c * GU_COLS, GU_COLS), GU_COLS)
        return [pltpu.make_async_copy(w.at[layer, expert, :, cols], gu.at[slot, k], gusem.at[slot, k])
                for k, w in enumerate((wg, wu))]

    def d_copies(d):
        layer, j, slot = d // d_chunks, d % d_chunks, (d % d_chunks) % DOWN_SLOTS
        return [pltpu.make_async_copy(wd.at[layer, k, :, columns(j)], dbuf.at[slot, k], dsem.at[slot, k]) for k in range(local)]

    kvw = KV * HEAD
    q_cols = heads * HEAD

    def proj(column, count):
        return gu.at[GU_SLOTS - 1, column // GU_COLS, :, pl.ds(column % GU_COLS, count)]

    def weight_copies(layer):
        pieces = range(q_cols // CHUNK)
        return [pltpu.make_async_copy(wk.at[layer], proj(q_cols, kvw), wsem.at[0]),
                pltpu.make_async_copy(wv.at[layer], proj(q_cols + kvw, kvw), wsem.at[1]),
                pltpu.make_async_copy(wo.at[layer], wo_b, wsem.at[2]),
                *(pltpu.make_async_copy(wq.at[layer, :, pl.ds(n * CHUNK, CHUNK)], proj(n * CHUNK, CHUNK), wsem.at[3 + n]) for n in pieces)]

    def kv_copies(layer, b):
        here = pl.ds(start + b * per_block, per_block)
        there = pl.ds(b * per_block, per_block)
        return [pltpu.make_async_copy(kc.at[layer, here], kbuf.at[there], kvsem.at[b, 0]),
                pltpu.make_async_copy(vc.at[layer, here], vbuf.at[there], kvsem.at[b, 1])]

    def start_projections(layer):
        copies = weight_copies(layer)
        for c in copies[3:] + copies[:2]:
            c.start()

    def start_caches(layer):
        for b in range(KV_BLOCKS):
            for c in kv_copies(layer, b):
                c.start()
        weight_copies(layer)[2].start()

    def start_attention(layer):
        start_projections(layer)
        start_caches(layer)

    def start_gate_up(layer):
        for i in range(GU_SLOTS - 1):
            for c in gu_copies(layer * gu_total + i):
                c.start()

    def start_down(layer):
        for j in range(DOWN_SLOTS):
            for c in d_copies(layer * d_chunks + j):
                c.start()

    first = [pltpu.make_async_copy(hid.at[pl.ds(start, toks)], acc_a, isem.at[0]),
             pltpu.make_async_copy(wr, wr_b, isem.at[1]),
             pltpu.make_async_copy(cos_t, cosb, isem.at[2]),
             pltpu.make_async_copy(sin_t, sinb, isem.at[3]),
             pltpu.make_async_copy(lens_h, lens, isem.at[4]),
             pltpu.make_async_copy(ids_h, ids, isem.at[5])]
    for c in first:
        c.start()
    start_projections(0)

    barrier = pltpu.get_barrier_semaphore()
    pl.semaphore_signal(barrier, inc=1, device_id={"ep": partner}, device_id_type=MESH)
    pl.semaphore_signal(barrier, inc=1, device_id={"ep": cross}, device_id_type=MESH)

    inside = (p > 0) & (p < pools - 1)
    for way in (-2, -1, 1, 2):
        @pl.when((p + way >= 0) & (p + way < pools))
        def _(way=way):
            pl.semaphore_signal(barrier, inc=1, device_id={"pool": p + way}, device_id_type=MESH)

    with jax.named_scope("firstwait"):
        for c in first:
            c.wait()

    start_caches(0)

    zeros = jnp.zeros(((16 - heads) * toks, HEAD), jnp.float32)
    for ref in (q2d, k2d, v2d):
        ref[pl.ds(heads * toks, (16 - heads) * toks), :] = zeros

    def spread(t, carry):
        where = pl.ds(t, 1)
        n = lens[start + t]
        cosr[where, :] = cosb[pl.ds(n, 1), :]
        sinr[where, :] = sinb[pl.ds(n, 1), :]
        for layer in range(layers):
            for k in range(2):
                id_b[layer, k, where, :] = jnp.full((1, LANES), ids[layer, k, start + t], jnp.int32)
        return carry

    with jax.named_scope("spread"):
        lax.fori_loop(0, toks, spread, 0)

    lane = lax.broadcasted_iota(jnp.int32, (16, seq2), 1)
    head_kv = jnp.where(lax.broadcasted_iota(jnp.int32, (16, seq2), 0) >= group, 1, 0)
    parity = (lane % KV) == head_kv
    scale = HEAD ** -0.5

    def layer_body(layer, carry):
        with jax.named_scope("qkv"):
            hidden = acc_a[...].astype(jnp.float32)
            h = normed(hidden).astype(jnp.bfloat16)
            copies = weight_copies(layer)
            for c in copies[3:] + copies[:2]:
                c.wait()
            cosine, sine = cosr[...], sinr[...]

            def rope(v):
                return (v * cosine + pltpu.roll(v, HEAD // 2, 1) * sine).astype(jnp.bfloat16).astype(jnp.float32)

            for n in range(heads * HEAD // CHUNK):
                qn = jnp.dot(h, proj(n * CHUNK, CHUNK)[...], preferred_element_type=jnp.float32)
                for k in range(CHUNK // HEAD):
                    head = n * (CHUNK // HEAD) + k
                    q2d[pl.ds(head * toks, toks), :] = rope(qn[:, k * HEAD:(k + 1) * HEAD])
            kv = jnp.dot(h, proj(q_cols, 2 * kvw)[...], preferred_element_type=jnp.float32)
            for j in range(KV):
                kj = rope(kv[:, j * HEAD:(j + 1) * HEAD])
                vj = kv[:, kvw + j * HEAD:kvw + (j + 1) * HEAD].astype(jnp.bfloat16).astype(jnp.float32)
                for k in range(group):
                    at = pl.ds((j * group + k) * toks, toks)
                    k2d[at, :] = kj
                    v2d[at, :] = vj

        @pl.when(layer == 0)
        def _():
            start_gate_up(0)

        for c in gu_copies(layer * gu_total + GU_SLOTS - 1):
            c.start()

        def score(first_token, ref):
            for k in range(GROUP):
                q = q2d[pl.ds(first_token + k, 16, stride=toks), :].astype(jnp.bfloat16)
                ref[k * 16:(k + 1) * 16, :] = lax.dot_general(q, kbuf[first_token + k], (((1,), (1,)), ((), ())),
                                                              preferred_element_type=jnp.float32)

        def mix(first_token, ref):
            weights, news, totals = [], [], []
            for k in range(GROUP):
                at = pl.ds(first_token + k, 16, stride=toks)
                n2 = lens[start + first_token + k] * KV
                s = jnp.where(parity & (lane < n2), ref[k * 16:(k + 1) * 16, :] * scale, -jnp.inf)
                s_new = jnp.sum(q2d[at, :] * k2d[at, :], axis=1, keepdims=True) * scale
                peak = jnp.maximum(jnp.max(s, axis=1, keepdims=True), s_new)
                w = jnp.exp(s - peak)
                w_new = jnp.exp(s_new - peak)
                totals.append(jnp.sum(w, axis=1, keepdims=True) + w_new)
                weights.append(w.astype(jnp.bfloat16))
                news.append(w_new.astype(jnp.bfloat16).astype(jnp.float32))
            sums = [jnp.dot(weights[k], vbuf[first_token + k], preferred_element_type=jnp.float32) for k in range(GROUP)]
            for k in range(GROUP):
                at = pl.ds(first_token + k, 16, stride=toks)
                o2d[at, :] = (sums[k] + news[k] * v2d[at, :]) / totals[k]

        with jax.named_scope("attn"):
            kv_copies(layer, 0)[0].wait()
            score(0, s_even)

            def attend(i, carry):
                kv_copies(layer, i)[1].wait()

                @pl.when(i + 1 < KV_BLOCKS)
                def _():
                    kv_copies(layer, i + 1)[0].wait()

                t = i * per_block
                score(t + GROUP, s_odd)
                mix(t, s_even)
                score((t + 2 * GROUP) % toks, s_even)
                mix(t + GROUP, s_odd)
                return carry

            lax.fori_loop(0, KV_BLOCKS, attend, 0)

        @pl.when(layer == 0)
        def _():
            start_down(0)

        with jax.named_scope("wo"):
            for head in range(heads):
                att[:, head * HEAD:(head + 1) * HEAD] = o2d[pl.ds(head * toks, toks), :].astype(jnp.bfloat16)
            copies[2].wait()
            for n in range(model // CHUNK):
                cols = slice(n * CHUNK, (n + 1) * CHUNK)
                a = acc_a[:, cols].astype(jnp.float32) + jnp.dot(att[...], wo_b[:, cols], preferred_element_type=jnp.float32)
                acc_a[:, cols] = a.astype(jnp.bfloat16)

        u = normed(acc_a[...].astype(jnp.float32)).astype(jnp.bfloat16)
        ubuf[layer, pl.ds(0, toks), :] = u

        def block(ref, b):
            return ref.at[layer, pl.ds(b * toks, toks)]

        def piece(b, h):
            return ubuf.at[layer, pl.ds(b * toks + h * half, half)]

        u_near = [remote(piece(0, h), piece(1, h), us.at[0, h], ur.at[layer, 0, h], "ep", partner) for h in range(2)]
        u_far = [remote(piece(0, h), piece(2, h), us.at[1, h], ur.at[layer, 1, h], "ep", cross) for h in range(2)]
        u_pass = [remote(piece(2, h), piece(3, h), us.at[2, h], ur.at[layer, 2, h], "ep", partner) for h in range(2)]
        g_near = remote(block(gbuf, 0), block(gbuf, 1), gs.at[0], gr.at[layer, 0], "ep", partner)
        g_far = remote(block(gbuf, 0), block(gbuf, 2), gs.at[1], gr.at[layer, 1], "ep", cross)
        g_pass = remote(block(gbuf, 2), block(gbuf, 3), gs.at[2], gr.at[layer, 2], "ep", partner)
        @pl.when((layer == 0) & inside)
        def _():
            pl.semaphore_wait(barrier, 5)

        @pl.when((layer == 0) & jnp.logical_not(inside))
        def _():
            pl.semaphore_wait(barrier, 4)

        for c in u_far + u_near:
            c.start()

        wl = wr_b[layer]
        hi = wl.astype(jnp.bfloat16).astype(jnp.float32)
        rest = wl - hi
        mid = rest.astype(jnp.bfloat16).astype(jnp.float32)
        low = rest - mid
        wide = jnp.concatenate([hi, mid, low, jnp.zeros((LANES - 3 * wl.shape[0], model), jnp.float32)], axis=0).astype(jnp.bfloat16)
        parts = lax.dot_general(u, wide, (((1,), (1,)), ((), ())), preferred_element_type=jnp.float32)
        logits = parts + pltpu.roll(parts, LANES - 8, 1) + pltpu.roll(parts, LANES - 16, 1)
        expert_lane = lax.broadcasted_iota(jnp.int32, (toks, LANES), 1)
        chosen = (id_b[layer, 0] == expert_lane) | (id_b[layer, 1] == expert_lane)
        logits = jnp.where(chosen, logits, -jnp.inf)
        ew = jnp.exp(logits - jnp.max(logits, axis=1, keepdims=True))
        gbuf[layer, pl.ds(0, toks), :] = ew / jnp.sum(ew, axis=1, keepdims=True)
        g_far.start()
        g_near.start()

        def gate_up(low, count, wait, release):
            def step(i, carry):
                g = layer * gu_total + i
                slot = i % GU_SLOTS
                if wait:
                    for c in gu_copies(g):
                        c.wait()
                for n in range(0, GU_COLS, PIECE):
                    tokens = ubuf[layer, low:low + count, :]
                    one = jnp.dot(tokens, gu[slot, 0, :, n:n + PIECE], preferred_element_type=jnp.float32)
                    three = jnp.dot(tokens, gu[slot, 1, :, n:n + PIECE], preferred_element_type=jnp.float32)
                    cols = pl.ds(pl.multiple_of((i % ff_chunks) * GU_COLS + n, PIECE), PIECE)
                    inner[i // ff_chunks, low:low + count, cols] = (jax.nn.silu(one) * three).astype(jnp.bfloat16)
                if release:
                    @pl.when(i + GU_SLOTS < gu_total)
                    def _():
                        for c in gu_copies(g + GU_SLOTS):
                            c.start()

                return carry

            return step

        with jax.named_scope("nearwait"):
            for c in u_near:
                c.wait_recv()

        with jax.named_scope("l"):
            lax.fori_loop(0, GU_SLOTS, gate_up(0, 2 * toks, True, False), 0)

        with jax.named_scope("farwait"):
            for h in range(2):
                u_far[h].wait_recv()
                u_pass[h].start()

        g_far.wait_recv()
        g_pass.start()
        with jax.named_scope("passwait"):
            for c in u_pass:
                c.wait_recv()

        with jax.named_scope("r"):
            lax.fori_loop(0, GU_SLOTS, gate_up(2 * toks, 2 * toks, False, True), 0)

        with jax.named_scope("main"):
            lax.fori_loop(GU_SLOTS, gu_total, gate_up(0, 4 * toks, True, True), 0)

        g_near.wait_recv()
        g_pass.wait_recv()
        gates = gbuf[layer]
        row_lane = lax.broadcasted_iota(jnp.int32, (rows, LANES), 1)
        for k in range(local):
            one = jnp.sum(jnp.where(row_lane == e * local + k, gates, 0.0), axis=1, keepdims=True)
            gsel[k] = jnp.broadcast_to(one, (rows, LANES))

        def near_l(j):
            return remote(stage.at[j, pl.ds(toks, toks)], part_l.at[layer, j], ps.at[j], pr.at[layer, j], "ep", partner)

        def near_m(j):
            return remote(stage.at[j, pl.ds(3 * toks, toks)], part_m.at[layer, j], ms.at[j], mr.at[layer, j], "ep", partner)

        def far_copy(j):
            return remote(merged.at[j], far.at[layer, j], fs.at[j], fr.at[layer, j], "ep", cross)

        def merge(j):
            near_m(j).wait_recv()
            merged[j] = stage[j, pl.ds(2 * toks, toks), :] + part_m[layer, j]
            far_copy(j).start()

        def combine(c):
            near_l(c).wait_recv()
            far_copy(c).wait_recv()
            total = (stage[c, pl.ds(0, toks), :] + part_l[layer, c]) + far[layer, c]
            x = (acc_a[:, columns(c)].astype(jnp.float32) + total).astype(jnp.bfloat16)
            acc_a[:, columns(c)] = x

            @pl.when(layer == layers - 1)
            def _():
                xg[p, c] = x
                store(p, c).start()

                for way in WAYS:
                    @pl.when((p + way >= 0) & (p + way < pools))
                    def _(way=way):
                        spread_out(p, c, way).start()

        def down(j, slot, low):
            terms = [None] * (DOWN_COLS // LANES)
            for k in range(local):
                y = jnp.dot(inner[k, low:low + 2 * toks, :], dbuf[slot, k], preferred_element_type=jnp.float32)
                y = y.astype(jnp.bfloat16).astype(jnp.float32)
                gate = gsel[k, low:low + 2 * toks, :]
                for n in range(len(terms)):
                    term = jnp.where(gate > 0.0, gate * y[:, n * LANES:(n + 1) * LANES], 0.0)
                    terms[n] = term if k == 0 else terms[n] + term
            for n in range(len(terms)):
                stage[j, low:low + 2 * toks, n * LANES:(n + 1) * LANES] = terms[n]

        def down_body(j, carry):
            d = layer * d_chunks + j

            for c in d_copies(d):
                c.wait()
            down(j, j % DOWN_SLOTS, 2 * toks)
            near_m(j).start()

            @pl.when(j > 0)
            def _():
                merge(j - 1)

            down(j, j % DOWN_SLOTS, 0)
            near_l(j).start()

            @pl.when(j + DOWN_SLOTS < d_chunks)
            def _():
                for c in d_copies(d + DOWN_SLOTS):
                    c.start()

            @pl.when((j == ATTENTION_AT) & (layer + 1 < layers))
            def _():
                start_attention(layer + 1)

            @pl.when(j >= LAG)
            def _():
                combine(j - LAG)

            return carry

        with jax.named_scope("down"):
            lax.fori_loop(0, d_chunks, down_body, 0)
            merge(d_chunks - 1)

        @pl.when(layer + 1 < layers)
        def _():
            start_gate_up(layer + 1)
            start_down(layer + 1)


        def last_ones(c, carry):
            combine(c)

            @pl.when(layer == layers - 1)
            def _():
                relay(c - RELAY_LAG)

            return carry

        with jax.named_scope("tail"):
            lax.fori_loop(d_chunks - LAG, d_chunks, last_ones, 0)

        for c in u_near + u_far + u_pass + [g_near, g_far, g_pass]:
            c.wait_send()

        def sent(j, carry):
            near_l(j).wait_send()
            near_m(j).wait_send()
            far_copy(j).wait_send()
            return carry

        lax.fori_loop(0, d_chunks, sent, 0)
        return carry

    def spread_out(origin, c, way, kind=None):
        at = xg.at[origin, c]
        return remote(at, at, zs.at[WAYS.index(way) if kind is None else kind, c], zr.at[origin, c], "pool", p + way)

    def store(origin, c):
        here = pl.ds(origin * toks, toks)
        return pltpu.make_async_copy(xg.at[origin, c], out.at[here, columns(c)], osem.at[0])

    def relay(c):
        @pl.when(p == 1)
        def _():
            received(3, c, 2)
            spread_out(3, c, -1, len(WAYS)).start()
            store(3, c).start()

        @pl.when(p == 2)
        def _():
            received(0, c, -2)
            spread_out(0, c, 1, len(WAYS)).start()
            store(0, c).start()

    def received(origin, c, way):
        spread_out(origin, c, way).wait_recv()

    lax.fori_loop(0, layers, layer_body, 0)

    def rest(c, carry):
        for step in range(1, pools):
            for origin, way in ((p - step, -1), (p + step, 1)):
                via_relay = ((p == 1) & (origin == 3)) | ((p == 2) & (origin == 0))

                @pl.when((origin >= 0) & (origin < pools) & jnp.logical_not(via_relay))
                def _(origin=origin, way=way):
                    received(origin, c, way)
                    store(origin, c).start()

        return carry

    def last_relays(c, carry):
        relay(c)
        return carry

    with jax.named_scope("relays"):
        lax.fori_loop(d_chunks - RELAY_LAG, d_chunks, last_relays, 0)

    with jax.named_scope("rest"):
        lax.fori_loop(0, d_chunks, rest, 0)

    def finish(c, carry):
        for way in WAYS:
            @pl.when((p + way >= 0) & (p + way < pools))
            def _(way=way):
                spread_out(p, c, way).wait_send()

        @pl.when(p == 1)
        def _():
            spread_out(3, c, -1, len(WAYS)).wait_send()

        @pl.when(p == 2)
        def _():
            spread_out(0, c, 1, len(WAYS)).wait_send()

        return carry

    with jax.named_scope("finish"):
        lax.fori_loop(0, d_chunks, finish, 0)
        pltpu.make_async_copy(out, out, osem.at[0]).wait()

def solution(mesh):
    pools = mesh.shape["pool"]

    def body(hidden, k_cache, v_cache, lengths, expert_ids, w_query, w_key, w_value, w_out, w_router, w_gate, w_up, w_down):
        layers, shard, seq, kv_heads, head = k_cache.shape
        model = hidden.shape[1]
        toks = shard // pools
        local, ff = w_gate.shape[1], w_gate.shape[3]
        heads = w_query.shape[2] // head
        dims = (layers, toks, model, ff, heads, local)
        cos_t, sin_t = rotary_tables(seq + 8)
        f32, bf16 = jnp.float32, jnp.bfloat16
        d_chunks = model // DOWN_COLS
        dma, vmem = pltpu.SemaphoreType.DMA, pltpu.VMEM
        scratch = [
            vmem((heads * head, model), bf16),
            vmem((toks, seq * kv_heads, head), bf16), vmem((toks, seq * kv_heads, head), bf16),
            vmem((GU_SLOTS, 2, model, GU_COLS), bf16), vmem((DOWN_SLOTS, local, ff, DOWN_COLS), bf16),
            vmem((layers, 4 * toks, model), bf16), vmem((local, 4 * toks, ff), bf16),
            vmem((d_chunks, 4 * toks, DOWN_COLS), f32),
            vmem((layers, d_chunks, toks, DOWN_COLS), f32), vmem((layers, d_chunks, toks, DOWN_COLS), f32),
            vmem((d_chunks, toks, DOWN_COLS), f32), vmem((layers, d_chunks, toks, DOWN_COLS), f32),
            vmem((pools, d_chunks, toks, DOWN_COLS), bf16), vmem((toks, model), bf16),
            vmem((16 * toks, head), f32), vmem((16 * toks, head), f32), vmem((16 * toks, head), f32), vmem((16 * toks, head), f32),
            vmem((GROUP * 16, seq * kv_heads), f32), vmem((GROUP * 16, seq * kv_heads), f32),
            vmem((toks, heads * head), bf16), vmem((layers, 4 * toks, LANES), f32), vmem((local, 4 * toks, LANES), f32),
            vmem((layers, w_router.shape[2], model), f32),
            pltpu.SMEM((shard,), jnp.int32), pltpu.SMEM((layers, 2, shard), jnp.int32),
            vmem(cos_t.shape, f32), vmem(sin_t.shape, f32), vmem((toks, head), f32), vmem((toks, head), f32),
            vmem((layers, 2, toks, LANES), jnp.int32),
            dma((3 + heads * head // CHUNK,)), dma((KV_BLOCKS, 2)), dma((GU_SLOTS, 2)), dma((DOWN_SLOTS, local)), dma((6,)),
            dma((3, 2)), dma((layers, 3, 2)), dma((3,)), dma((layers, 3)),
            dma((d_chunks,)), dma((layers, d_chunks)), dma((d_chunks,)), dma((layers, d_chunks)),
            dma((d_chunks,)), dma((layers, d_chunks)), dma((len(WAYS) + 1, d_chunks)), dma((pools, d_chunks)), dma((1,)),
        ]
        anyw = pl.BlockSpec(memory_space=pl.ANY)
        return pl.pallas_call(
            functools.partial(kernel, dims),
            out_shape=jax.ShapeDtypeStruct((shard, model), bf16),
            in_specs=[anyw] * 15,
            out_specs=anyw,
            scratch_shapes=scratch,
            compiler_params=pltpu.CompilerParams(collective_id=0, has_side_effects=True, vmem_limit_bytes=67043328),
            name="decode",
        )(lengths, jnp.swapaxes(expert_ids, 1, 2), hidden,
          k_cache.reshape(layers, shard, seq * kv_heads, head), v_cache.reshape(layers, shard, seq * kv_heads, head),
          w_query, w_key, w_value, w_out, jnp.swapaxes(w_router, 1, 2), jnp.asarray(cos_t), jnp.asarray(sin_t),
          w_gate, w_up, w_down)

    rows_spec = ("dp", "ep")
    in_specs = (P(rows_spec, None), P(None, rows_spec), P(None, rows_spec), P(rows_spec), P(None, rows_spec, None), P(), P(), P(), P(), P(), P(None, "ep"), P(None, "ep"), P(None, "ep"))
    return jax.shard_map(body, mesh=mesh, in_specs=in_specs, out_specs=P(rows_spec, None), check_vma=False)
```

```python
import functools
import math

import jax
import jax.numpy as jnp
import numpy as np
from jax import lax
from jax.experimental import pallas as pl
from jax.experimental.pallas import tpu as pltpu
from jax.sharding import PartitionSpec as P

EPSILON = 1e-6
ROPE_BASE = 10000.0
MESH = pl.DeviceIdType.MESH
HEAD = 128
KV = 2
LANES = 128
CHUNK = 512
GU_COLS = 1024
GU_SLOTS = 4
PIECE = 256
DOWN_SLOTS = 3
DOWN_COLS = 256
KV_BLOCKS = 4
GROUP = 8
LAG = 3
ATTENTION_AT = 3
WAYS = (-2, 2, -1, 1)
RELAY_LAG = 3


def rotary_tables(size):
    half = HEAD // 2
    freqs = np.float32(ROPE_BASE) ** (np.float32(-2.0) * np.arange(half, dtype=np.float32) / np.float32(HEAD))
    angle = np.arange(size, dtype=np.float32)[:, None] * freqs[None, :].astype(np.float32)
    cosine = np.cos(angle).astype(np.float32)
    sine = np.sin(angle).astype(np.float32)
    return np.concatenate([cosine, cosine], 1), np.concatenate([-sine, sine], 1)


def normed(values):
    return values * lax.rsqrt(jnp.mean(values * values, axis=-1, keepdims=True) + EPSILON)


def kernel(dims, lens_h, ids_h, hid, kc, vc, wq, wk, wv, wo, wr, cos_t, sin_t, wg, wu, wd, out,
           wo_b, kbuf, vbuf, gu, dbuf, ubuf, inner, stage, part_l, part_m, merged, far, xg, acc_a,
           q2d, k2d, v2d, o2d, s_even, s_odd, att, gbuf, gsel, wr_b, lens, ids, cosb, sinb, cosr, sinr, id_b,
           wsem, kvsem, gusem, dsem, isem, us, ur, gs, gr, ps, pr, ms, mr, fs, fr, zs, zr, osem):
    layers, toks, model, ff, heads, local = dims
    e = lax.axis_index("ep")
    p = lax.axis_index("pool")
    pools = 4
    partner = e + 1 - 2 * (e % 2)
    cross = (e + 2) % 4
    start = p * toks
    ff_chunks = ff // GU_COLS
    gu_total = local * ff_chunks
    d_chunks = model // DOWN_COLS
    rows = 4 * toks
    half = toks // 2
    group = heads // KV
    seq2 = kbuf.shape[1]
    per_block = toks // KV_BLOCKS

    def remote(src, dst, ssem, rsem, axis, index):
        return pltpu.make_async_remote_copy(src_ref=src, dst_ref=dst, send_sem=ssem, recv_sem=rsem,
                                            device_id={axis: index}, device_id_type=MESH)

    def columns(j):
        return pl.ds(pl.multiple_of(j * DOWN_COLS, DOWN_COLS), DOWN_COLS)

    def gu_copies(g):
        layer, i, slot = g // gu_total, g % gu_total, (g % gu_total) % GU_SLOTS
        expert, c = i // ff_chunks, i % ff_chunks
        cols = pl.ds(pl.multiple_of(c * GU_COLS, GU_COLS), GU_COLS)
        return [pltpu.make_async_copy(w.at[layer, expert, :, cols], gu.at[slot, k], gusem.at[slot, k])
                for k, w in enumerate((wg, wu))]

    def d_copies(d):
        layer, j, slot = d // d_chunks, d % d_chunks, (d % d_chunks) % DOWN_SLOTS
        return [pltpu.make_async_copy(wd.at[layer, k, :, columns(j)], dbuf.at[slot, k], dsem.at[slot, k]) for k in range(local)]

    kvw = KV * HEAD
    q_cols = heads * HEAD

    def proj(column, count):
        return gu.at[GU_SLOTS - 1, column // GU_COLS, :, pl.ds(column % GU_COLS, count)]

    def weight_copies(layer):
        pieces = range(q_cols // CHUNK)
        return [pltpu.make_async_copy(wk.at[layer], proj(q_cols, kvw), wsem.at[0]),
                pltpu.make_async_copy(wv.at[layer], proj(q_cols + kvw, kvw), wsem.at[1]),
                pltpu.make_async_copy(wo.at[layer], wo_b, wsem.at[2]),
                *(pltpu.make_async_copy(wq.at[layer, :, pl.ds(n * CHUNK, CHUNK)], proj(n * CHUNK, CHUNK), wsem.at[3 + n]) for n in pieces)]

    def kv_copies(layer, b):
        here = pl.ds(start + b * per_block, per_block)
        there = pl.ds(b * per_block, per_block)
        return [pltpu.make_async_copy(kc.at[layer, here], kbuf.at[there], kvsem.at[b, 0]),
                pltpu.make_async_copy(vc.at[layer, here], vbuf.at[there], kvsem.at[b, 1])]

    def start_projections(layer):
        copies = weight_copies(layer)
        for c in copies[3:] + copies[:2]:
            c.start()

    def start_caches(layer):
        for b in range(KV_BLOCKS):
            for c in kv_copies(layer, b):
                c.start()
        weight_copies(layer)[2].start()

    def start_attention(layer):
        start_projections(layer)
        start_caches(layer)

    def start_gate_up(layer):
        for i in range(GU_SLOTS - 1):
            for c in gu_copies(layer * gu_total + i):
                c.start()

    def start_down(layer):
        for j in range(DOWN_SLOTS):
            for c in d_copies(layer * d_chunks + j):
                c.start()

    first = [pltpu.make_async_copy(hid.at[pl.ds(start, toks)], acc_a, isem.at[0]),
             pltpu.make_async_copy(wr, wr_b, isem.at[1]),
             pltpu.make_async_copy(cos_t, cosb, isem.at[2]),
             pltpu.make_async_copy(sin_t, sinb, isem.at[3]),
             pltpu.make_async_copy(lens_h, lens, isem.at[4]),
             pltpu.make_async_copy(ids_h, ids, isem.at[5])]
    for c in first:
        c.start()
    start_projections(0)

    barrier = pltpu.get_barrier_semaphore()
    pl.semaphore_signal(barrier, inc=1, device_id={"ep": partner}, device_id_type=MESH)
    pl.semaphore_signal(barrier, inc=1, device_id={"ep": cross}, device_id_type=MESH)

    inside = (p > 0) & (p < pools - 1)
    for way in (-2, -1, 1, 2):
        @pl.when((p + way >= 0) & (p + way < pools))
        def _(way=way):
            pl.semaphore_signal(barrier, inc=1, device_id={"pool": p + way}, device_id_type=MESH)

    for c in first:
        c.wait()
    start_caches(0)

    zeros = jnp.zeros(((16 - heads) * toks, HEAD), jnp.float32)
    for ref in (q2d, k2d, v2d):
        ref[pl.ds(heads * toks, (16 - heads) * toks), :] = zeros

    def spread(t, carry):
        where = pl.ds(t, 1)
        n = lens[start + t]
        cosr[where, :] = cosb[pl.ds(n, 1), :]
        sinr[where, :] = sinb[pl.ds(n, 1), :]
        for layer in range(layers):
            for k in range(2):
                id_b[layer, k, where, :] = jnp.full((1, LANES), ids[layer, k, start + t], jnp.int32)
        return carry

    lax.fori_loop(0, toks, spread, 0, unroll=8)

    lane = lax.broadcasted_iota(jnp.int32, (16, seq2), 1)
    head_kv = jnp.where(lax.broadcasted_iota(jnp.int32, (16, seq2), 0) >= group, 1, 0)
    parity = (lane % KV) == head_kv
    scale = HEAD ** -0.5

    def layer_body(layer, carry):
        hidden = acc_a[...].astype(jnp.float32)
        h = normed(hidden).astype(jnp.bfloat16)
        copies = weight_copies(layer)
        for c in copies[3:] + copies[:2]:
            c.wait()
        cosine, sine = cosr[...], sinr[...]

        def rope(v):
            return (v * cosine + pltpu.roll(v, HEAD // 2, 1) * sine).astype(jnp.bfloat16).astype(jnp.float32)

        for n in range(heads * HEAD // CHUNK):
            qn = jnp.dot(h, proj(n * CHUNK, CHUNK)[...], preferred_element_type=jnp.float32)
            for k in range(CHUNK // HEAD):
                head = n * (CHUNK // HEAD) + k
                q2d[pl.ds(head * toks, toks), :] = rope(qn[:, k * HEAD:(k + 1) * HEAD])
        kv = jnp.dot(h, proj(q_cols, 2 * kvw)[...], preferred_element_type=jnp.float32)
        for j in range(KV):
            kj = rope(kv[:, j * HEAD:(j + 1) * HEAD])
            vj = kv[:, kvw + j * HEAD:kvw + (j + 1) * HEAD].astype(jnp.bfloat16).astype(jnp.float32)
            for k in range(group):
                at = pl.ds((j * group + k) * toks, toks)
                k2d[at, :] = kj
                v2d[at, :] = vj

        @pl.when(layer == 0)
        def _():
            start_gate_up(0)

        for c in gu_copies(layer * gu_total + GU_SLOTS - 1):
            c.start()

        def score(first_token, ref):
            for k in range(GROUP):
                q = q2d[pl.ds(first_token + k, 16, stride=toks), :].astype(jnp.bfloat16)
                ref[k * 16:(k + 1) * 16, :] = lax.dot_general(q, kbuf[first_token + k], (((1,), (1,)), ((), ())),
                                                              preferred_element_type=jnp.float32)

        def mix(first_token, ref):
            weights, news, totals = [], [], []
            for k in range(GROUP):
                at = pl.ds(first_token + k, 16, stride=toks)
                n2 = lens[start + first_token + k] * KV
                s = jnp.where(parity & (lane < n2), ref[k * 16:(k + 1) * 16, :] * scale, -jnp.inf)
                s_new = jnp.sum(q2d[at, :] * k2d[at, :], axis=1, keepdims=True) * scale
                peak = jnp.maximum(jnp.max(s, axis=1, keepdims=True), s_new)
                w = jnp.exp(s - peak)
                w_new = jnp.exp(s_new - peak)
                totals.append(jnp.sum(w, axis=1, keepdims=True) + w_new)
                weights.append(w.astype(jnp.bfloat16))
                news.append(w_new.astype(jnp.bfloat16).astype(jnp.float32))
            sums = [jnp.dot(weights[k], vbuf[first_token + k], preferred_element_type=jnp.float32) for k in range(GROUP)]
            for k in range(GROUP):
                at = pl.ds(first_token + k, 16, stride=toks)
                o2d[at, :] = (sums[k] + news[k] * v2d[at, :]) / totals[k]

        kv_copies(layer, 0)[0].wait()
        score(0, s_even)

        def attend(i, carry):
            kv_copies(layer, i)[1].wait()

            @pl.when(i + 1 < KV_BLOCKS)
            def _():
                kv_copies(layer, i + 1)[0].wait()

            t = i * per_block
            score(t + GROUP, s_odd)
            mix(t, s_even)
            score((t + 2 * GROUP) % toks, s_even)
            mix(t + GROUP, s_odd)
            return carry

        lax.fori_loop(0, KV_BLOCKS, attend, 0)

        for head in range(heads):
            att[:, head * HEAD:(head + 1) * HEAD] = o2d[pl.ds(head * toks, toks), :].astype(jnp.bfloat16)
        copies[2].wait()
        for n in range(model // CHUNK):
            cols = slice(n * CHUNK, (n + 1) * CHUNK)
            a = acc_a[:, cols].astype(jnp.float32) + jnp.dot(att[...], wo_b[:, cols], preferred_element_type=jnp.float32)
            acc_a[:, cols] = a.astype(jnp.bfloat16)

        u = normed(acc_a[...].astype(jnp.float32)).astype(jnp.bfloat16)
        ubuf[layer, pl.ds(0, toks), :] = u

        def block(ref, b):
            return ref.at[layer, pl.ds(b * toks, toks)]

        def piece(b, h):
            return ubuf.at[layer, pl.ds(b * toks + h * half, half)]

        u_near = [remote(piece(0, h), piece(1, h), us.at[0, h], ur.at[layer, 0, h], "ep", partner) for h in range(2)]
        u_far = [remote(piece(0, h), piece(2, h), us.at[1, h], ur.at[layer, 1, h], "ep", cross) for h in range(2)]
        u_pass = [remote(piece(2, h), piece(3, h), us.at[2, h], ur.at[layer, 2, h], "ep", partner) for h in range(2)]
        g_near = remote(block(gbuf, 0), block(gbuf, 1), gs.at[0], gr.at[layer, 0], "ep", partner)
        g_far = remote(block(gbuf, 0), block(gbuf, 2), gs.at[1], gr.at[layer, 1], "ep", cross)
        g_pass = remote(block(gbuf, 2), block(gbuf, 3), gs.at[2], gr.at[layer, 2], "ep", partner)
        @pl.when((layer == 0) & inside)
        def _():
            pl.semaphore_wait(barrier, 5)

        @pl.when((layer == 0) & jnp.logical_not(inside))
        def _():
            pl.semaphore_wait(barrier, 4)

        for c in u_far + u_near:
            c.start()

        wl = wr_b[layer]
        hi = wl.astype(jnp.bfloat16).astype(jnp.float32)
        rest = wl - hi
        mid = rest.astype(jnp.bfloat16).astype(jnp.float32)
        low = rest - mid
        wide = jnp.concatenate([hi, mid, low, jnp.zeros((LANES - 3 * wl.shape[0], model), jnp.float32)], axis=0).astype(jnp.bfloat16)
        parts = lax.dot_general(u, wide, (((1,), (1,)), ((), ())), preferred_element_type=jnp.float32)
        logits = parts + pltpu.roll(parts, LANES - 8, 1) + pltpu.roll(parts, LANES - 16, 1)
        expert_lane = lax.broadcasted_iota(jnp.int32, (toks, LANES), 1)
        chosen = (id_b[layer, 0] == expert_lane) | (id_b[layer, 1] == expert_lane)
        logits = jnp.where(chosen, logits, -jnp.inf)
        ew = jnp.exp(logits - jnp.max(logits, axis=1, keepdims=True))
        gbuf[layer, pl.ds(0, toks), :] = ew / jnp.sum(ew, axis=1, keepdims=True)
        g_far.start()
        g_near.start()

        def rows_of(i, low, count):
            slot = i % GU_SLOTS
            for n in range(0, GU_COLS, PIECE):
                tokens = ubuf[layer, low:low + count, :]
                one = jnp.dot(tokens, gu[slot, 0, :, n:n + PIECE], preferred_element_type=jnp.float32)
                three = jnp.dot(tokens, gu[slot, 1, :, n:n + PIECE], preferred_element_type=jnp.float32)
                cols = pl.ds(pl.multiple_of((i % ff_chunks) * GU_COLS + n, PIECE), PIECE)
                inner[i // ff_chunks, low:low + count, cols] = (jax.nn.silu(one) * three).astype(jnp.bfloat16)

        def near_step(i, carry):
            for c in gu_copies(layer * gu_total + i):
                c.wait()
            rows_of(i, 0, 2 * toks)
            return carry

        def far_step(m, carry):
            for i in (2 * m, 2 * m + 1):
                rows_of(i, 2 * toks, 2 * toks)
                for c in gu_copies(layer * gu_total + i + GU_SLOTS):
                    c.start()
            return carry

        def all_step(i, carry):
            for c in gu_copies(layer * gu_total + i):
                c.wait()
            rows_of(i, 0, 4 * toks)
            return carry

        for c in u_near:
            c.wait_recv()
        lax.fori_loop(0, GU_SLOTS, near_step, 0)
        for h in range(2):
            u_far[h].wait_recv()
            u_pass[h].start()
        g_far.wait_recv()
        g_pass.start()
        for c in u_pass:
            c.wait_recv()
        lax.fori_loop(0, GU_SLOTS // 2, far_step, 0)
        @pl.when(layer == 0)
        def _():
            start_down(0)

        lax.fori_loop(GU_SLOTS, gu_total, all_step, 0)

        g_near.wait_recv()
        g_pass.wait_recv()
        gates = gbuf[layer]
        row_lane = lax.broadcasted_iota(jnp.int32, (rows, LANES), 1)
        for k in range(local):
            one = jnp.sum(jnp.where(row_lane == e * local + k, gates, 0.0), axis=1, keepdims=True)
            gsel[k] = jnp.broadcast_to(one, (rows, LANES))

        def near_l(j):
            return remote(stage.at[j, pl.ds(toks, toks)], part_l.at[layer, j], ps.at[j], pr.at[layer, j], "ep", partner)

        def near_m(j):
            return remote(stage.at[j, pl.ds(3 * toks, toks)], part_m.at[layer, j], ms.at[j], mr.at[layer, j], "ep", partner)

        def far_copy(j):
            return remote(merged.at[j], far.at[layer, j], fs.at[j], fr.at[layer, j], "ep", cross)

        def merge(j):
            near_m(j).wait_recv()
            merged[j] = stage[j, pl.ds(2 * toks, toks), :] + part_m[layer, j]
            far_copy(j).start()

        def combine(c):
            near_l(c).wait_recv()
            far_copy(c).wait_recv()
            total = (stage[c, pl.ds(0, toks), :] + part_l[layer, c]) + far[layer, c]
            x = (acc_a[:, columns(c)].astype(jnp.float32) + total).astype(jnp.bfloat16)
            acc_a[:, columns(c)] = x

            @pl.when(layer == layers - 1)
            def _():
                xg[p, c] = x
                store(p, c).start()

                for way in WAYS:
                    @pl.when((p + way >= 0) & (p + way < pools))
                    def _(way=way):
                        spread_out(p, c, way).start()

        def down(j, slot, low):
            terms = [None] * (DOWN_COLS // LANES)
            for k in range(local):
                y = jnp.dot(inner[k, low:low + 2 * toks, :], dbuf[slot, k], preferred_element_type=jnp.float32)
                y = y.astype(jnp.bfloat16).astype(jnp.float32)
                gate = gsel[k, low:low + 2 * toks, :]
                for n in range(len(terms)):
                    term = jnp.where(gate > 0.0, gate * y[:, n * LANES:(n + 1) * LANES], 0.0)
                    terms[n] = term if k == 0 else terms[n] + term
            for n in range(len(terms)):
                stage[j, low:low + 2 * toks, n * LANES:(n + 1) * LANES] = terms[n]

        def down_body(j, carry):
            d = layer * d_chunks + j

            for c in d_copies(d):
                c.wait()
            down(j, j % DOWN_SLOTS, 2 * toks)
            near_m(j).start()

            @pl.when(j > 0)
            def _():
                merge(j - 1)

            down(j, j % DOWN_SLOTS, 0)
            near_l(j).start()

            @pl.when(j + DOWN_SLOTS < d_chunks)
            def _():
                for c in d_copies(d + DOWN_SLOTS):
                    c.start()

            @pl.when((j == ATTENTION_AT) & (layer + 1 < layers))
            def _():
                start_attention(layer + 1)

            @pl.when((j >= LAG) & (layer == layers - 1))
            def _():
                combine(j - LAG)

            return carry

        lax.fori_loop(0, d_chunks, down_body, 0)
        merge(d_chunks - 1)

        @pl.when(layer + 1 < layers)
        def _():
            start_gate_up(layer + 1)
            start_down(layer + 1)


        def last_ones(c, carry):
            combine(c)

            @pl.when(layer == layers - 1)
            def _():
                relay(c - RELAY_LAG)

            return carry

        lax.fori_loop((d_chunks - LAG) * (layer // (layers - 1)), d_chunks, last_ones, 0)

        for c in u_near + u_far + u_pass + [g_near, g_far, g_pass]:
            c.wait_send()

        def sent(j, carry):
            near_l(j).wait_send()
            near_m(j).wait_send()
            far_copy(j).wait_send()
            return carry

        lax.fori_loop(0, d_chunks, sent, 0)
        return carry

    def spread_out(origin, c, way, kind=None):
        at = xg.at[origin, c]
        return remote(at, at, zs.at[WAYS.index(way) if kind is None else kind, c], zr.at[origin, c], "pool", p + way)

    def store(origin, c):
        here = pl.ds(origin * toks, toks)
        return pltpu.make_async_copy(xg.at[origin, c], out.at[here, columns(c)], osem.at[0])

    def relay(c):
        @pl.when(p == 1)
        def _():
            received(3, c, 2)
            spread_out(3, c, -1, len(WAYS)).start()
            store(3, c).start()

        @pl.when(p == 2)
        def _():
            received(0, c, -2)
            spread_out(0, c, 1, len(WAYS)).start()
            store(0, c).start()

    def received(origin, c, way):
        spread_out(origin, c, way).wait_recv()

    lax.fori_loop(0, layers, layer_body, 0)

    def rest(c, carry):
        for step in range(1, pools):
            for origin, way in ((p - step, -1), (p + step, 1)):
                via_relay = ((p == 1) & (origin == 3)) | ((p == 2) & (origin == 0))

                @pl.when((origin >= 0) & (origin < pools) & jnp.logical_not(via_relay))
                def _(origin=origin, way=way):
                    received(origin, c, way)
                    store(origin, c).start()

        return carry

    def last_relays(c, carry):
        relay(c)
        return carry

    lax.fori_loop(d_chunks - RELAY_LAG, d_chunks, last_relays, 0)
    lax.fori_loop(0, d_chunks, rest, 0)

    def finish(c, carry):
        for way in WAYS:
            @pl.when((p + way >= 0) & (p + way < pools))
            def _(way=way):
                spread_out(p, c, way).wait_send()

        @pl.when(p == 1)
        def _():
            spread_out(3, c, -1, len(WAYS)).wait_send()

        @pl.when(p == 2)
        def _():
            spread_out(0, c, 1, len(WAYS)).wait_send()

        return carry

    lax.fori_loop(0, d_chunks, finish, 0)
    pltpu.make_async_copy(out, out, osem.at[0]).wait()


def solution(mesh):
    pools = mesh.shape["pool"]

    def body(hidden, k_cache, v_cache, lengths, expert_ids, w_query, w_key, w_value, w_out, w_router, w_gate, w_up, w_down):
        layers, shard, seq, kv_heads, head = k_cache.shape
        model = hidden.shape[1]
        toks = shard // pools
        local, ff = w_gate.shape[1], w_gate.shape[3]
        heads = w_query.shape[2] // head
        dims = (layers, toks, model, ff, heads, local)
        cos_t, sin_t = rotary_tables(seq + 8)
        f32, bf16 = jnp.float32, jnp.bfloat16
        d_chunks = model // DOWN_COLS
        dma, vmem = pltpu.SemaphoreType.DMA, pltpu.VMEM
        scratch = [
            vmem((heads * head, model), bf16),
            vmem((toks, seq * kv_heads, head), bf16), vmem((toks, seq * kv_heads, head), bf16),
            vmem((GU_SLOTS, 2, model, GU_COLS), bf16), vmem((DOWN_SLOTS, local, ff, DOWN_COLS), bf16),
            vmem((layers, 4 * toks, model), bf16), vmem((local, 4 * toks, ff), bf16),
            vmem((d_chunks, 4 * toks, DOWN_COLS), f32),
            vmem((layers, d_chunks, toks, DOWN_COLS), f32), vmem((layers, d_chunks, toks, DOWN_COLS), f32),
            vmem((d_chunks, toks, DOWN_COLS), f32), vmem((layers, d_chunks, toks, DOWN_COLS), f32),
            vmem((pools, d_chunks, toks, DOWN_COLS), bf16), vmem((toks, model), bf16),
            vmem((16 * toks, head), f32), vmem((16 * toks, head), f32), vmem((16 * toks, head), f32), vmem((16 * toks, head), f32),
            vmem((GROUP * 16, seq * kv_heads), f32), vmem((GROUP * 16, seq * kv_heads), f32),
            vmem((toks, heads * head), bf16), vmem((layers, 4 * toks, LANES), f32), vmem((local, 4 * toks, LANES), f32),
            vmem((layers, w_router.shape[2], model), f32),
            pltpu.SMEM((shard,), jnp.int32), pltpu.SMEM((layers, 2, shard), jnp.int32),
            vmem(cos_t.shape, f32), vmem(sin_t.shape, f32), vmem((toks, head), f32), vmem((toks, head), f32),
            vmem((layers, 2, toks, LANES), jnp.int32),
            dma((3 + heads * head // CHUNK,)), dma((KV_BLOCKS, 2)), dma((GU_SLOTS, 2)), dma((DOWN_SLOTS, local)), dma((6,)),
            dma((3, 2)), dma((layers, 3, 2)), dma((3,)), dma((layers, 3)),
            dma((d_chunks,)), dma((layers, d_chunks)), dma((d_chunks,)), dma((layers, d_chunks)),
            dma((d_chunks,)), dma((layers, d_chunks)), dma((len(WAYS) + 1, d_chunks)), dma((pools, d_chunks)), dma((1,)),
        ]
        anyw = pl.BlockSpec(memory_space=pl.ANY)
        return pl.pallas_call(
            functools.partial(kernel, dims),
            out_shape=jax.ShapeDtypeStruct((shard, model), bf16),
            in_specs=[anyw] * 15,
            out_specs=anyw,
            scratch_shapes=scratch,
            compiler_params=pltpu.CompilerParams(collective_id=0, has_side_effects=True, vmem_limit_bytes=67043328),
            name="decode",
        )(lengths, jnp.swapaxes(expert_ids, 1, 2), hidden,
          k_cache.reshape(layers, shard, seq * kv_heads, head), v_cache.reshape(layers, shard, seq * kv_heads, head),
          w_query, w_key, w_value, w_out, jnp.swapaxes(w_router, 1, 2), jnp.asarray(cos_t), jnp.asarray(sin_t),
          w_gate, w_up, w_down)

    rows_spec = ("dp", "ep")
    in_specs = (P(rows_spec, None), P(None, rows_spec), P(None, rows_spec), P(rows_spec), P(None, rows_spec, None), P(), P(), P(), P(), P(), P(None, "ep"), P(None, "ep"), P(None, "ep"))
    return jax.shard_map(body, mesh=mesh, in_specs=in_specs, out_specs=P(rows_spec, None), check_vma=False)
```
